32 devices in a mesh: ka: 8 (over z, core), band: 4 (over y, x).
Axes of the slice: x: 2, y: 2, z: 4, core: 2. Of those that a mesh axis runs over, the one named last changes fastest.
Arguments:
- occ_rows: bfloat16 [8, 2048, 128], P('ka', 'band'), may hold values from -0.5 to 0.5
- vir_rows: bfloat16 [8, 2048, 896], P('ka', 'band'), may hold values from -0.1875 to 0.1875
- trial_vectors: float32 [8, 2, 128, 896], P('ka', None, None, 'band'), may hold values from -6 to 6
- occ_energy: float32 [8, 128], P('ka'), may hold values from -1.2 to -0.3
- vir_energy: float32 [8, 896], P('ka', 'band'), may hold values from 0.1 to 1.5
- coulomb: bfloat16 [2048, 2048], P('band'), may hold values from -0.09375 to 0.09375
- exch_kernel: bfloat16 [8, 2048, 2048], P(None, 'band'), as said below
- minus_table: int32 [8, 8], replicated, may hold values from 0 to 7, as said below
Outputs:
- sigma_vectors: float32 [8, 2, 128, 896], P('ka', None, None, 'band')
The draws below stay inside these ranges and needn't reach their ends.
Inputs may be any that keep to these rules, and one draw needn't show every extreme that they name: minus_table[k, q] is the k-point k - q on a group of 8 k-points: every row and every column holds each index once, and one q gives minus_table[k, q] == k for every k. Each exch_kernel[q] is symmetric.
All inputs are finite; a program needn't handle non-finite values.
Results may differ from the reference program's by a relative error of at most 0.0051.
Values may be sent and summed in bfloat16 or wider, within the bound.
A program may use at most 128 MiB of HBM per device.

```python
import jax
import jax.numpy as jnp
from jax import lax

NOCC = 128
NVIR = 896
NAUX = 2048
NVEC = 2
NK = 8


def draw_minus_table(key, part):
    labels = jax.random.permutation(jax.random.fold_in(key, 11), NK).astype(jnp.int32)
    difference = (labels[:, None] - labels[None, :]) % NK
    inverse = jnp.argsort(labels).astype(jnp.int32)
    return inverse[difference].astype(jnp.int32)


def draw_exch_kernel(key, part):
    spread = jnp.sqrt(jnp.float32(NOCC) / jnp.float32(NK * NAUX))
    base = jax.random.normal(jax.random.fold_in(key, 3), (NK, NAUX, NAUX), jnp.float32)
    symmetric = (base + jnp.transpose(base, (0, 2, 1))) * 0.7071
    return (symmetric * spread).astype(jnp.bfloat16)


def levels(stream_key, shape, split, smallest, high):
    factor_of = 1.0
    for position, blocks in split:
        draws = jax.random.uniform(jax.random.fold_in(jax.random.fold_in(stream_key, 6), position), (blocks,), jnp.float32, smallest / len(split), high / len(split))
        factor_of = factor_of * jnp.repeat(jnp.exp(draws), shape[position] // blocks).reshape((-1,) + (1,) * (len(shape) - 1 - position))
    return factor_of


def normal_values(key, shape, scale, reach, shards=(), held_as=jnp.bfloat16):
    result = scale * jax.random.normal(key, shape, jnp.float32)
    if shards:
        result = result * levels(key, shape, shards, -0.22, 0.18)
    return jnp.clip(result, -reach, reach).astype(held_as)


def setup_inputs(seed: int = 0) -> dict:
    key_list = jax.random.split(jax.random.key(seed), 9)
    occ_rows = normal_values(key_list[0], (NK, NAUX, NOCC), NOCC ** -0.5, 0.5, ((0, 8), (1, 4)))
    vir_rows = normal_values(key_list[1], (NK, NAUX, NVIR), NVIR ** -0.5, 0.1875, ((0, 8), (1, 4)))
    trial_vectors = normal_values(key_list[2], (NK, NVEC, NOCC, NVIR), 1.0, 6.0, ((0, 8), (3, 4)), jnp.float32)
    occ_energy = jnp.clip(-1.2 + 0.90000004 * jax.random.uniform(key_list[3], (NK, NOCC), jnp.float32) ** levels(key_list[3], (NK, NOCC), ((0, 8),), -0.2, 0.2), -1.2, -0.3)
    vir_energy = jnp.clip(0.1 + 1.4 * jax.random.uniform(key_list[4], (NK, NVIR), jnp.float32) ** levels(key_list[4], (NK, NVIR), ((0, 8), (1, 4)), -0.2, 0.2), 0.1, 1.5)
    coulomb = normal_values(key_list[5], (NAUX, NAUX), (NK * NAUX // 4) ** -0.5, 0.09375, ((0, 4),))
    exch_kernel = draw_exch_kernel(jax.random.fold_in(key_list[8], 71), 0)
    minus_table = draw_minus_table(jax.random.fold_in(key_list[8], 71), 0)
    return dict(occ_rows=occ_rows, vir_rows=vir_rows, trial_vectors=trial_vectors, occ_energy=occ_energy, vir_energy=vir_energy, coulomb=coulomb, exch_kernel=exch_kernel, minus_table=minus_table)


def reference(occ_rows, vir_rows, trial_vectors, occ_energy, vir_energy, coulomb, exch_kernel, minus_table):
    highest = lax.Precision.HIGHEST
    trial_half = trial_vectors.astype(jnp.bfloat16)

    def build_pairs(kpoint):
        occ_here = occ_rows[kpoint].astype(jnp.float32)
        vir_here = vir_rows[kpoint].astype(jnp.float32)
        mixed_rows = jnp.einsum("ri,via->vra", occ_here, trial_half[kpoint].astype(jnp.float32), precision=highest)
        mixed_rows = mixed_rows.astype(jnp.bfloat16)
        pair_block = jnp.einsum("vra,na->vrn", mixed_rows.astype(jnp.float32), vir_here, precision=highest)
        density_here = jnp.sum(mixed_rows.astype(jnp.float32) * vir_here[None], axis=2)
        return pair_block.astype(jnp.bfloat16), density_here

    pair_blocks, densities = lax.map(build_pairs, jnp.arange(NK, dtype=jnp.int32))
    density_half = jnp.sum(densities, axis=0).astype(jnp.bfloat16)
    potential = jnp.einsum("vn,rn->vr", density_half.astype(jnp.float32), coulomb.astype(jnp.float32), precision=highest)

    def build_sigma(kpoint):
        def add_transfer(running, momentum):
            source = minus_table[kpoint, momentum]
            weighted = pair_blocks[source].astype(jnp.float32) * exch_kernel[momentum].astype(jnp.float32)[None]
            return running + weighted, None

        screened, unused = lax.scan(add_transfer, jnp.zeros((NVEC, NAUX, NAUX), jnp.float32), jnp.arange(NK, dtype=jnp.int32))
        screened = screened.astype(jnp.bfloat16)
        vir_here = vir_rows[kpoint].astype(jnp.float32)
        product = jnp.einsum("vrn,na->vra", screened.astype(jnp.float32), vir_here, precision=highest)
        weights = (2.0 * potential[:, :, None] * vir_here[None] - product).astype(jnp.bfloat16)
        coupled = jnp.einsum("ri,vra->via", occ_rows[kpoint].astype(jnp.float32), weights.astype(jnp.float32), precision=highest)
        energy_gaps = vir_energy[kpoint][None, :] - occ_energy[kpoint][:, None]
        return energy_gaps[None] * trial_vectors[kpoint] + coupled

    return lax.map(build_sigma, jnp.arange(NK, dtype=jnp.int32))
```

```python
import functools

import jax
import jax.numpy as jnp
from jax import lax
from jax.experimental import pallas as pl
from jax.experimental.pallas import tpu as pltpu
from jax.sharding import PartitionSpec as P

F32 = jnp.float32
BF16 = jnp.bfloat16
CHUNK = 16
SPAN = 512


def dot_nt(left, right, **options):
    return lax.dot_general(
        left, right, (((1,), (1,)), ((), ())), preferred_element_type=F32, **options
    )


def aligned(start, size):
    return pl.ds(pl.multiple_of(start, size), size)


def kernel(
    kpoints,
    bands,
    vectors,
    occ,
    vir,
    trial,
    coulomb,
    exch,
    table,
    out,
    trial_full,
    vir_turned,
    half_own,
    half_all,
    occ_tile,
    dens_all,
    dens_band,
    potential,
    coulomb_here,
    exch_tile,
    pairs,
    screened,
    sums_send,
    sums_slot,
    coupling,
    sigma_send,
    sigma_recv,
    local_sem,
    trial_sem,
    point_sem,
    occ_sem,
    occ_pass_sem,
    half_send_sem,
    half_recv_sem,
    half_pass_sem,
    dens_sem,
    dens_band_sem,
    sums_send_sem,
    sums_recv_sem,
    sigma_sem,
):
    me = lax.axis_index("ka")
    band = lax.axis_index("band")
    groups = kpoints // 2
    count = groups // 2
    group = lax.div(me, 2)
    core = lax.rem(me, 2)
    sibling = me + 1 - 2 * core
    pair = lax.div(group, 2)
    side = lax.rem(group, 2)
    partner = group + 1 - 2 * side
    rows, occupied = occ.shape
    columns = trial.shape[1]
    block = rows // groups
    piece = rows // 2
    width = bands * piece
    near_x = band + 1 - 2 * lax.rem(band, 2)
    near_y = lax.rem(band + 2, bands)
    corner = bands - 1 - band
    others = (corner, near_x, near_y)

    def tile_of(k):
        return lax.rem(k, 2) * groups + lax.div(k, 2)

    def remote(source, target, send, recv, device):
        return pltpu.make_async_remote_copy(
            src_ref=source,
            dst_ref=target,
            send_sem=send,
            recv_sem=recv,
            device_id=device,
            device_id_type=pl.DeviceIdType.MESH,
        )

    def arrival(target, recv):
        return remote(target, target, recv, recv, (sibling, band))

    exch_copies = []
    for part in range(bands):
        copy = pltpu.make_async_copy(
            exch.at[
                :,
                aligned((2 * pair + core) * block, block),
                aligned(part * rows + side * piece, piece),
            ],
            exch_tile.at[:, :, pl.ds(part * piece, piece)],
            local_sem.at[1 + part],
        )
        copy.start()
        exch_copies.append(copy)
    coulomb_copy = pltpu.make_async_copy(coulomb, coulomb_here, local_sem.at[0])
    coulomb_copy.start()

    own_columns = aligned(band * columns, columns)
    trial_full[:, own_columns, :] = trial[...].astype(BF16)

    barrier = pltpu.get_barrier_semaphore()
    for peer in others:
        pl.semaphore_signal(
            barrier, inc=1, device_id=(me, peer), device_id_type=pl.DeviceIdType.MESH
        )
    for step in range(1, kpoints):
        pl.semaphore_signal(
            barrier,
            inc=1,
            device_id=(lax.rem(me + step, kpoints), band),
            device_id_type=pl.DeviceIdType.MESH,
        )
    pl.semaphore_wait(barrier, len(others) + kpoints - 1)

    started = []

    def send(copy):
        copy.start()
        started.append(copy)
        return copy

    trial_copies = []
    for v in range(vectors):
        trial_copies.append(
            [
                send(
                    remote(
                        trial_full.at[v, own_columns],
                        trial_full.at[v, own_columns],
                        trial_sem.at[0, v, way],
                        trial_sem.at[1, v, way],
                        (me, peer),
                    )
                )
                for way, peer in enumerate(others)
            ]
        )

    def piece_of(owner):
        return aligned(owner * piece, piece)

    mine = tile_of(me)
    for step in range(1, groups):
        peer = lax.rem(group + step, groups)
        send(
            remote(
                occ.at[aligned(lax.rem(peer, 2) * piece, piece)],
                occ_tile.at[mine, piece_of(band)],
                point_sem.at[0, step],
                point_sem.at[1, group],
                (peer * 2 + core, band),
            )
        )
    occ_tile[mine, piece_of(band), :] = occ[aligned(side * piece, piece), :]

    def occ_out(source_group):
        tile = core * groups + source_group
        here = occ_tile.at[tile, piece_of(band)]
        for way, peer in ((1, near_x), (2, near_y)):
            send(
                remote(
                    here,
                    here,
                    occ_sem.at[0, source_group, way],
                    occ_sem.at[1, source_group, way],
                    (me, peer),
                )
            )
        occ_pass(source_group, 0, band)

    def occ_pass(source_group, way, owner):
        here = occ_tile.at[core * groups + source_group, piece_of(owner)]
        send(
            remote(
                here,
                here,
                occ_pass_sem.at[0, source_group, way],
                occ_pass_sem.at[1, source_group, way],
                (sibling, band),
            )
        )

    tile_order = [lax.rem(group + step, groups) for step in range(groups)]
    occ_out(tile_order[0])

    def own_half(v):
        for copy in trial_copies[v]:
            copy.wait_recv()
        half_own[v] = jnp.dot(vir[...], trial_full[v], preferred_element_type=F32).astype(BF16)
        lines = pl.ds(v * block, block)
        own_block = 2 * pair + core
        half_all[me, lines, :] = half_own[v, aligned(own_block * block, block), :]
        slot = 0
        destinations = []
        for step in range(1, count):
            other = lax.rem(pair + step, count)
            near = lax.select(other > pair, 2 * other, 2 * other + 1)
            destinations += [(2 * other + side_core, near * 2 + side_core) for side_core in range(2)]
        destinations += [(2 * pair + side_core, partner * 2 + side_core) for side_core in range(2)]
        destinations.append((2 * pair + 1 - core, sibling))
        for slot, (which, device) in enumerate(destinations):
            send(
                remote(
                    half_own.at[v, aligned(which * block, block)],
                    half_all.at[me, lines],
                    half_send_sem.at[v, slot],
                    half_recv_sem.at[v, me],
                    (device, band),
                )
            )

    for v in range(vectors):
        own_half(v)

    ones = jnp.ones((8, occupied), F32)
    occ_wide = occ[...].astype(F32)
    density = jnp.concatenate(
        [
            dot_nt(ones, occ_wide * half_own[v].astype(F32), precision=lax.Precision.HIGHEST)[:1]
            for v in range(vectors)
        ],
        axis=0,
    )
    dens_all[me] = density
    dens_copies = [
        send(
            remote(
                dens_all.at[me],
                dens_all.at[me],
                dens_sem.at[0, step],
                dens_sem.at[1, step],
                (lax.rem(me + step, kpoints), band),
            )
        )
        for step in range(1, kpoints)
    ]

    for source_group in tile_order[1:]:
        arrival(
            occ_tile.at[core * groups + source_group, piece_of(band)],
            point_sem.at[1, source_group],
        ).wait_recv()
        occ_out(source_group)

    vir_turned[...] = vir[...].T

    passes = []

    def take_halves(v, source_group, forward):
        for owner_core in range(2):
            source = source_group * 2 + owner_core
            here = half_all.at[source, pl.ds(v * block, block)]
            arrival(here, half_recv_sem.at[v, source]).wait_recv()
            if forward is None:
                continue
            copy = remote(
                here,
                here,
                half_pass_sem.at[v, source],
                half_recv_sem.at[v, source],
                (partner * 2 + core, band),
            )
            pl.when(forward == 1)(copy.start)
            passes.append((copy, forward))

    far_groups = []
    for step in range(groups - 2):
        low = lax.rem(2 * pair + 2 + step, groups)
        high = lax.rem(2 * pair + 2 * groups - 1 - step, groups)
        source_group = lax.select(2 * pair < count, low, high)
        forward = lax.select(source_group < 2 * pair, 1 - side, side)
        far_groups.append((source_group, forward))

    def take_all_halves(v):
        there = half_all.at[sibling, pl.ds(v * block, block)]
        arrival(there, half_recv_sem.at[v, sibling]).wait_recv()
        take_halves(v, partner, None)
        for source_group, forward in far_groups:
            take_halves(v, source_group, forward)

    def occ_in(position):
        source_group = tile_order[position]
        tile = core * groups + source_group
        first = position < groups // 2
        for way, peer, onward in ((1, near_x, near_y), (2, near_y, near_x)):
            here = occ_tile.at[tile, piece_of(peer)]
            arrival(here, occ_sem.at[1, source_group, way]).wait_recv()
            if first == (way == 1):
                send(
                    remote(
                        here,
                        here,
                        occ_sem.at[0, source_group, 3],
                        occ_sem.at[1, source_group, 3],
                        (me, onward),
                    )
                )
            occ_pass(source_group, way, peer)

    take_all_halves(0)
    for position in range(groups):
        occ_in(position)

    for copy in dens_copies:
        copy.wait_recv()
    density = dens_all[0]
    for k in range(1, kpoints):
        density += dens_all[k]
    dens_band[band] = density
    dens_band_copies = [
        send(
            remote(
                dens_band.at[band],
                dens_band.at[band],
                dens_band_sem.at[0, way],
                dens_band_sem.at[1, way],
                (me, peer),
            )
        )
        for way, peer in enumerate(others)
    ]
    for v in range(1, vectors):
        take_all_halves(v)
    for source_group in tile_order:
        here = occ_tile.at[core * groups + source_group, piece_of(corner)]
        arrival(here, occ_sem.at[1, source_group, 3]).wait_recv()
        occ_pass(source_group, 3, corner)
    for copy in exch_copies:
        copy.wait()

    def make_pairs(source):
        pairs[source] = dot_nt(half_all[source], occ_tile[tile_of(source)])

    for source_group in tile_order:
        make_pairs(source_group * 2 + core)

    for copy in dens_band_copies:
        copy.wait_recv()
    coulomb_copy.wait()
    spread = jnp.zeros((16 - vectors, rows), F32)
    total = jnp.zeros((rows, 16), F32)
    for part in range(bands):
        here = jnp.concatenate([dens_band[part], spread], axis=0).astype(BF16)
        total += dot_nt(coulomb_here[:, part * rows : (part + 1) * rows], here)
    potential[:, :16] = total

    for source_group in tile_order:
        tile = (1 - core) * groups + source_group
        for way, owner in enumerate((band, near_x, near_y, corner)):
            arrival(
                occ_tile.at[tile, piece_of(owner)], occ_pass_sem.at[1, source_group, way]
            ).wait_recv()
        make_pairs(source_group * 2 + 1 - core)

    def screen(v, targets):
        sources = [[table[target, q] for q in range(kpoints)] for target in targets]
        spans = width // SPAN

        def add_rows(index, carry):
            start = lax.div(index, spans) * CHUNK
            here = aligned(start, CHUNK)
            there = pl.ds(pl.multiple_of(v * block + start, CHUNK), CHUNK)
            across = aligned(lax.rem(index, spans) * SPAN, SPAN)
            totals = [jnp.zeros((CHUNK, SPAN), F32) for _ in targets]
            for q in range(kpoints):
                factor = exch_tile[q, here, across].astype(F32)
                for n in range(len(targets)):
                    totals[n] += pairs[sources[n][q], there, across] * factor
            for n in range(len(targets)):
                screened[n, here, across] = totals[n].astype(BF16)
            return carry

        lax.fori_loop(0, block // CHUNK * spans, add_rows, 0)
        return [
            jnp.dot(screened[n], occ_tile[tile_of(target)], preferred_element_type=F32)
            for n, target in enumerate(targets)
        ]

    own_block = 2 * pair + core
    lower = 2 * pair
    higher = groups - 2 - lower
    outward = lax.select(side == 0, higher, lower)

    def send_sums(v):
        for step in range(groups - 1):
            rising = lax.select(step <= higher, groups - 1 - step, step - higher - 1)
            falling = lax.select(step <= lower, step, groups + lower - step)
            target_group = lax.select(side == 0, rising, falling)
            through = step < outward
            gather = step > outward
            totals = screen(v, [target_group * 2 + n for n in range(2)])
            for n in range(2):
                target = target_group * 2 + n
                total = totals[n]
                sending = sums_send.at[v, step, n]
                slot = lax.select(
                    through,
                    2 * groups + target,
                    2 * own_block + lax.select(gather, jnp.int32(0), side),
                )
                device = lax.select(through, partner * 2 + core, target)

                @pl.when(gather)
                def _(total=total, target=target, sending=sending):
                    before = sums_slot.at[v, 2 * groups + target]
                    arrival(before, sums_recv_sem.at[v, 2 * groups + target]).wait_recv()
                    sending[...] = (total + before[...].astype(F32)).astype(BF16)

                @pl.when(jnp.logical_not(gather))
                def _(total=total, sending=sending):
                    sending[...] = total.astype(BF16)

                send(
                    remote(
                        sending,
                        sums_slot.at[v, slot],
                        sums_send_sem.at[v, step, n],
                        sums_recv_sem.at[v, slot],
                        (device, band),
                    )
                )
        totals = screen(v, [sibling, me])
        sending = sums_send.at[v, groups - 1, 0]
        sending[...] = totals[0].astype(BF16)
        slot = 2 * own_block + side
        send(
            remote(
                sending,
                sums_slot.at[v, slot],
                sums_send_sem.at[v, groups - 1, 0],
                sums_recv_sem.at[v, slot],
                (sibling, band),
            )
        )
        sums_slot[v, slot] = totals[1].astype(BF16)

    sigma_copies = []

    def sigma_of(v, peer):
        return jnp.dot(
            vir_turned[aligned(peer * columns, columns), :],
            coupling[v],
            preferred_element_type=F32,
        )

    def make_sigma(v):
        def take(slot):
            arrival(sums_slot.at[v, slot], sums_recv_sem.at[v, slot]).wait_recv()

        take(2 * (2 * pair + core) + 1 - side)
        for part in range(2):
            take(2 * (2 * pair + 1 - core) + part)
        for step in range(count):
            other = lax.rem(pair + step, count)
            for side_core in range(2):
                which = 2 * other + side_core
                if step:
                    take(2 * which)
                total = sums_slot[v, 2 * which].astype(F32)
                if not step:
                    total += sums_slot[v, 2 * which + 1].astype(F32)
                lines = aligned(which * block, block)
                direct = 2.0 * potential[lines, v : v + 1] * occ[lines, :].astype(F32)
                coupling[v, lines, :] = (direct - total).astype(BF16)
        copies = []
        for way, peer in enumerate(others):
            sigma_send[v, way] = sigma_of(v, peer).astype(BF16)
            copies.append(
                send(
                    remote(
                        sigma_send.at[v, way],
                        sigma_recv.at[v, way],
                        sigma_sem.at[0, v, way],
                        sigma_sem.at[1, v, way],
                        (me, peer),
                    )
                )
            )
        sigma_copies.append(copies)
        out[v] = sigma_of(v, band)

    for v in range(vectors):
        send_sums(v)
    for v in range(vectors):
        make_sigma(v)
    for v in range(vectors):
        result = out[v]
        for way, copy in enumerate(sigma_copies[v]):
            copy.wait_recv()
            result += sigma_recv[v, way].astype(F32)
        out[v] = result

    for copy in started:
        copy.wait_send()
    for copy, forward in passes:
        pl.when(forward == 1)(copy.wait_send)


def coupled_part(kpoints, bands, occ, vir, trial, coulomb, exch, table, vectors):
    rows, occupied = occ.shape
    columns = trial.shape[1]
    groups = kpoints // 2
    block = rows // groups
    width = bands * rows // 2
    vmem = pl.BlockSpec(memory_space=pltpu.VMEM)
    hbm = pl.BlockSpec(memory_space=pl.ANY)
    smem = pl.BlockSpec(memory_space=pltpu.SMEM)
    dma = pltpu.SemaphoreType.DMA
    return pl.pallas_call(
        functools.partial(kernel, kpoints, bands, vectors),
        out_shape=jax.ShapeDtypeStruct(trial.shape, F32),
        in_specs=[vmem, vmem, vmem, hbm, hbm, smem],
        out_specs=vmem,
        scratch_shapes=[
            pltpu.VMEM((vectors, bands * columns, occupied), BF16),
            pltpu.VMEM((bands * columns, rows), BF16),
            pltpu.VMEM((vectors, rows, occupied), BF16),
            pltpu.VMEM((kpoints, vectors * block, occupied), BF16),
            pltpu.VMEM((kpoints, width, occupied), BF16),
            pltpu.VMEM((kpoints, vectors, rows), F32),
            pltpu.VMEM((bands, vectors, rows), F32),
            pltpu.VMEM((rows, 128), F32),
            pltpu.VMEM(coulomb.shape, BF16),
            pltpu.VMEM((kpoints, block, width), BF16),
            pltpu.VMEM((kpoints, vectors * block, width), F32),
            pltpu.VMEM((2, block, width), BF16),
            pltpu.VMEM((vectors, groups, 2, block, occupied), BF16),
            pltpu.VMEM((vectors, 2 * groups + kpoints, block, occupied), BF16),
            pltpu.VMEM((vectors, rows, occupied), BF16),
            pltpu.VMEM((vectors, bands - 1, columns, occupied), BF16),
            pltpu.VMEM((vectors, bands - 1, columns, occupied), BF16),
            dma((1 + bands,)),
            dma((2, vectors, bands)),
            dma((2, groups)),
            dma((2, groups, bands)),
            dma((2, groups, bands)),
            dma((vectors, groups + 1)),
            dma((vectors, kpoints)),
            dma((vectors, kpoints)),
            dma((2, kpoints)),
            dma((2, bands)),
            dma((vectors, groups, 2)),
            dma((vectors, 2 * groups + kpoints)),
            dma((2, vectors, bands)),
        ],
        compiler_params=pltpu.CompilerParams(
            collective_id=0, has_side_effects=True, vmem_limit_bytes=60 * 2**20
        ),
        name="coupled",
    )(occ, vir, trial, coulomb, exch, table)


def per_device(
    occ_rows, vir_rows, trial_vectors, occ_energy, vir_energy, coulomb, exch_kernel, minus_table
):
    kpoints = lax.axis_size("ka")
    bands = lax.axis_size("band")
    vectors = trial_vectors.shape[1]
    trial_turned = jnp.swapaxes(trial_vectors[0], 1, 2)
    coupled = coupled_part(
        kpoints,
        bands,
        occ_rows[0],
        vir_rows[0],
        trial_turned,
        coulomb,
        exch_kernel,
        minus_table,
        vectors,
    )
    energy_gaps = vir_energy[0][:, None] - occ_energy[0][None, :]
    return jnp.swapaxes(energy_gaps[None] * trial_turned + coupled, 1, 2)[None]


def solution(mesh):
    in_specs = (
        P("ka", "band", None),
        P("ka", "band", None),
        P("ka", None, None, "band"),
        P("ka", None),
        P("ka", "band"),
        P("band", None),
        P(None, "band", None),
        P(),
    )
    out_specs = P("ka", None, None, "band")
    return jax.shard_map(
        per_device, mesh=mesh, in_specs=in_specs, out_specs=out_specs, check_vma=False
    )
```

```python
import functools

import jax
import jax.numpy as jnp
from jax import lax
from jax.experimental import pallas as pl
from jax.experimental.pallas import tpu as pltpu
from jax.sharding import PartitionSpec as P

F32 = jnp.float32
BF16 = jnp.bfloat16
CHUNK = 16
SPAN = 512


def dot_nt(left, right, **options):
    return lax.dot_general(
        left, right, (((1,), (1,)), ((), ())), preferred_element_type=F32, **options
    )


def aligned(start, size):
    return pl.ds(pl.multiple_of(start, size), size)


def kernel(
    kpoints,
    bands,
    vectors,
    occ_given,
    vir_given,
    trial_given,
    occ_energy_given,
    vir_energy_given,
    coulomb,
    exch,
    table_given,
    out,
    occ,
    vir,
    trial,
    occ_energy,
    vir_energy,
    table,
    gaps,
    exch_wide,
    trial_full,
    vir_turned,
    half_own,
    half_all,
    occ_tile,
    dens_all,
    dens_band,
    potential,
    coulomb_here,
    exch_tile,
    pairs,
    held,
    sums_send,
    sums_slot,
    coupling,
    sigma_send,
    sigma_recv,
    local_sem,
    trial_sem,
    point_sem,
    occ_send_sem,
    occ_sem,
    occ_pass_sem,
    half_send_sem,
    half_recv_sem,
    half_pass_sem,
    dens_sem,
    dens_band_sem,
    sums_send_sem,
    sums_recv_sem,
    sigma_sem,
):
    me = lax.axis_index("ka")
    band = lax.axis_index("band")
    groups = kpoints // 2
    count = groups // 2
    group = lax.div(me, 2)
    core = lax.rem(me, 2)
    sibling = me + 1 - 2 * core
    pair = lax.div(group, 2)
    side = lax.rem(group, 2)
    partner = group + 1 - 2 * side
    rows, occupied = occ.shape
    columns = trial.shape[1]
    block = rows // groups
    piece = rows // 2
    width = bands * piece
    near_x = band + 1 - 2 * lax.rem(band, 2)
    near_y = lax.rem(band + 2, bands)
    corner = bands - 1 - band
    others = (corner, near_x, near_y)

    def tile_of(k):
        return lax.rem(k, 2) * groups + lax.div(k, 2)

    def remote(source, target, send, recv, device):
        return pltpu.make_async_remote_copy(
            src_ref=source,
            dst_ref=target,
            send_sem=send,
            recv_sem=recv,
            device_id=device,
            device_id_type=pl.DeviceIdType.MESH,
        )

    def arrival(target, recv):
        return remote(target, target, recv, recv, (sibling, band))

    def drain(held, sem):
        pltpu.make_async_copy(held, held, sem).wait()

    barrier = pltpu.get_barrier_semaphore()
    for peer in others:
        pl.semaphore_signal(
            barrier, inc=1, device_id=(me, peer), device_id_type=pl.DeviceIdType.MESH
        )
    for step in range(1, kpoints):
        pl.semaphore_signal(
            barrier,
            inc=1,
            device_id=(lax.rem(me + step, kpoints), band),
            device_id_type=pl.DeviceIdType.MESH,
        )

    load_copies = []
    for given, here in (
        (trial_given, trial),
        (occ_given, occ),
        (vir_given, vir),
        (table_given, table),
        (occ_energy_given, occ_energy),
        (vir_energy_given, vir_energy),
    ):
        copy = pltpu.make_async_copy(given, here, local_sem.at[2 + len(load_copies)])
        copy.start()
        load_copies.append(copy)
    trial_load, occ_load, vir_load, *other_loads = load_copies
    for part in range(bands):
        pltpu.make_async_copy(
            exch.at[
                :,
                aligned((2 * pair + core) * block, block),
                aligned(part * rows + side * piece, piece),
            ],
            exch_tile.at[:, :, pl.ds(part * piece, piece)],
            local_sem.at[1],
        ).start()
    coulomb_copy = pltpu.make_async_copy(coulomb, coulomb_here, local_sem.at[0])
    coulomb_copy.start()

    own_columns = aligned(band * columns, columns)
    trial_load.wait()
    trial_full[:, own_columns, :] = trial[...].astype(BF16)
    pl.semaphore_wait(barrier, len(others) + kpoints - 1)

    for v in range(vectors):
        for peer in others:
            remote(
                trial_full.at[v, own_columns],
                trial_full.at[v, own_columns],
                trial_sem.at[vectors],
                trial_sem.at[v],
                (me, peer),
            ).start()

    def piece_of(owner):
        return aligned(owner * piece, piece)

    far_groups = []
    for step in range(groups - 2):
        low = lax.rem(2 * pair + 2 + step, groups)
        high = lax.rem(2 * pair + 2 * groups - 1 - step, groups)
        far_groups.append(lax.select(2 * pair < count, low, high))
    order = [group, partner] + far_groups

    mine = tile_of(me)
    occ_load.wait()
    point_copies = []
    for step, peer in enumerate(order[1:]):
        copy = remote(
            occ.at[aligned(lax.rem(peer, 2) * piece, piece)],
            occ_tile.at[mine, piece_of(band)],
            point_sem.at[0, step],
            point_sem.at[1, group],
            (peer * 2 + core, band),
        )
        copy.start()
        point_copies.append(copy)
    occ_tile[mine, piece_of(band), :] = occ[aligned(side * piece, piece), :]

    def occ_out(source_group):
        tile = core * groups + source_group
        here = occ_tile.at[tile, piece_of(band)]
        for way, peer in ((1, near_x), (2, near_y)):
            remote(
                here,
                here,
                occ_send_sem.at[0],
                occ_sem.at[source_group, way - 1],
                (me, peer),
            ).start()
        occ_pass(source_group, 0, band).start()

    def occ_pass(source_group, way, owner):
        here = occ_tile.at[core * groups + source_group, piece_of(owner)]
        return remote(
            here,
            here,
            occ_pass_sem.at[0],
            occ_pass_sem.at[1 + way // (bands - 1)],
            (sibling, band),
        )

    occ_out(group)
    vir_load.wait()
    vir_turned[...] = vir[...].T
    for copy in other_loads:
        copy.wait()
    turned = jnp.broadcast_to(vir_energy[...], (occupied, columns)).T
    gaps[...] = turned - occ_energy[...]
    drain(exch_tile, local_sem.at[1])

    def widen(k, carry):
        exch_wide[k] = exch_tile[k].astype(F32)
        return carry

    lax.fori_loop(0, kpoints, widen, 0)

    def take_point(source_group):
        arrival(
            occ_tile.at[core * groups + source_group, piece_of(band)],
            point_sem.at[1, source_group],
        ).wait_recv()
        occ_out(source_group)

    def own_half(v):
        drain(sigma_recv.at[v], trial_sem.at[v])
        half_own[v] = jnp.dot(vir[...], trial_full[v], preferred_element_type=F32).astype(BF16)
        lines = pl.ds(v * block, block)
        own_block = 2 * pair + core
        half_all[me, lines, :] = half_own[v, aligned(own_block * block, block), :]
        destinations = []
        for step in range(1, count):
            other = lax.rem(pair + step, count)
            near = lax.select(other > pair, 2 * other, 2 * other + 1)
            destinations += [(2 * other + side_core, near * 2 + side_core) for side_core in range(2)]
        destinations += [(2 * pair + side_core, partner * 2 + side_core) for side_core in range(2)]
        destinations.append((2 * pair + 1 - core, sibling))
        for which, device in destinations:
            remote(
                half_own.at[v, aligned(which * block, block)],
                half_all.at[me, lines],
                half_send_sem.at[0],
                half_recv_sem.at[v, me],
                (device, band),
            ).start()

    take_point(partner)
    for v in range(vectors):
        own_half(v)

    for source_group in far_groups:
        take_point(source_group)

    def half_pass(v, position, owner_core):
        source = far_groups[position] * 2 + owner_core
        here = half_all.at[source, pl.ds(v * block, block)]
        return remote(
            here,
            here,
            half_pass_sem.at[v, position, owner_core],
            half_recv_sem.at[v, source],
            (partner * 2 + core, band),
        )

    def take_half(v, source):
        here = half_all.at[source, pl.ds(v * block, block)]
        arrival(here, half_recv_sem.at[v, source]).wait_recv()

    def passing(source_group):
        return lax.select(source_group < 2 * pair, 1 - side, side) == 1

    def take_far(v, position):
        for owner_core in range(2):
            take_half(v, far_groups[position] * 2 + owner_core)
            pl.when(passing(far_groups[position]))(half_pass(v, position, owner_core).start)

    def occ_turn(position):
        source_group = order[position]
        tile = core * groups + source_group
        if position < groups // 2:
            owner, onward = near_x, near_y
        else:
            owner, onward = near_y, near_x
        here = occ_tile.at[tile, piece_of(owner)]
        return remote(
            here,
            here,
            occ_send_sem.at[0],
            occ_sem.at[source_group, 2],
            (me, onward),
        )

    def occ_in(position):
        source_group = order[position]
        tile = core * groups + source_group
        for way, owner in ((1, near_x), (2, near_y)):
            here = occ_tile.at[tile, piece_of(owner)]
            arrival(here, occ_sem.at[source_group, way - 1]).wait_recv()
            if (position < groups // 2) == (way == 1):
                occ_turn(position).start()
            occ_pass(source_group, way, owner).start()

    inner = lax.select(2 * pair < count, side, 1 - side) == 1

    @pl.when(inner)
    def _():
        turns = [(v, far) for v in range(vectors) for far in range(groups - 2)]
        for position in range(max(groups, len(turns))):
            if position < groups:
                occ_in(position)
            if position < len(turns):
                take_far(*turns[position])

    @pl.when(jnp.logical_not(inner))
    def _():
        for position in range(groups):
            occ_in(position)

    ones = jnp.ones((8, occupied), F32)
    occ_wide = occ[...].astype(F32)
    dens_all[me] = jnp.concatenate(
        [
            dot_nt(ones, occ_wide * half_own[v].astype(F32), precision=lax.Precision.HIGHEST)[:1]
            for v in range(vectors)
        ],
        axis=0,
    )
    for step in range(1, kpoints):
        remote(
            dens_all.at[me],
            dens_all.at[me],
            dens_sem.at[0],
            dens_sem.at[1],
            (lax.rem(me + step, kpoints), band),
        ).start()

    def take_corner(position):
        source_group = order[position]
        here = occ_tile.at[core * groups + source_group, piece_of(corner)]
        arrival(here, occ_sem.at[source_group, 2]).wait_recv()
        occ_pass(source_group, bands - 1, corner).start()

    def take_halves(v):
        take_half(v, sibling)
        for source in (partner * 2, partner * 2 + 1):
            take_half(v, source)

        @pl.when(jnp.logical_not(inner))
        def _():
            for far in range(groups - 2):
                take_far(v, far)

    def make_pairs(v, owners):
        lines = pl.ds(v * block, block)
        for source in range(kpoints):
            tile = tile_of(source)
            if len(owners) == bands:
                pairs[source, lines] = dot_nt(half_all[source, lines], occ_tile[tile])
                continue
            for owner in owners:
                part = piece_of(owner)
                pairs[source, lines, part] = dot_nt(
                    half_all[source, lines], occ_tile[tile, part]
                )

    def sum_density():
        drain(dens_all.at[pl.ds(0, kpoints - 1)], dens_sem.at[1])
        density = dens_all[0]
        for k in range(1, kpoints):
            density += dens_all[k]
        dens_band[band] = density
        for peer in others:
            remote(
                dens_band.at[band],
                dens_band.at[band],
                dens_band_sem.at[0],
                dens_band_sem.at[1],
                (me, peer),
            ).start()

    def make_potential():
        drain(dens_band.at[pl.ds(0, bands - 1)], dens_band_sem.at[1])
        coulomb_copy.wait()
        spread = jnp.zeros((16 - vectors, rows), F32)
        total = jnp.zeros((rows, 16), F32)
        for part in range(bands):
            here = jnp.concatenate([dens_band[part], spread], axis=0).astype(BF16)
            total += dot_nt(coulomb_here[:, part * rows : (part + 1) * rows], here)
        potential[:, :16] = total

    def screen(v, targets, spans):
        sources = [[table[target, q] for q in range(kpoints)] for target in targets]
        results = [jnp.zeros((block, occupied), F32) for _ in targets]
        for across, span in spans:
            chunks = [[] for _ in targets]
            for start in range(0, block, CHUNK):
                totals = [jnp.zeros((CHUNK, span), F32) for _ in targets]
                for q in range(kpoints):
                    factor = exch_wide[q, pl.ds(start, CHUNK), across]
                    for n in range(len(targets)):
                        there = pl.ds(v * block + start, CHUNK)
                        totals[n] += pairs[sources[n][q], there, across] * factor
                for n in range(len(targets)):
                    chunks[n].append(totals[n].astype(BF16))
            for n, target in enumerate(targets):
                results[n] += jnp.dot(
                    jnp.concatenate(chunks[n], axis=0),
                    occ_tile[tile_of(target), across],
                    preferred_element_type=F32,
                )
        return results

    whole = [(pl.ds(first, SPAN), SPAN) for first in range(0, width, SPAN)]
    early = [(piece_of(owner), piece) for owner in (band, near_x, near_y)]
    late = [(piece_of(corner), piece)]

    own_block = 2 * pair + core
    lower = 2 * pair
    higher = groups - 2 - lower
    outward = lax.select(side == 0, higher, lower)

    def far_target(step):
        rising = lax.select(step <= higher, groups - 1 - step, step - higher - 1)
        falling = lax.select(step <= lower, step, groups + lower - step)
        return lax.select(side == 0, rising, falling)

    def sums_to(v, step, n, device, slot, recv):
        remote(
            sums_send.at[v, step, n],
            sums_slot.at[v, slot],
            sums_send_sem.at[v],
            sums_recv_sem.at[v, recv],
            (device, band),
        ).start()

    def screen_far(v, step, spans, before=None):
        target_group = far_target(step)
        totals = screen(v, [target_group * 2 + n for n in range(2)], spans)
        for n in range(2):
            held[v, step, n] = totals[n] if before is None else held[v, step, n] + totals[n]

    def send_far(v, step):
        target_group = far_target(step)
        through = step < outward

        @pl.when(step <= outward)
        def _():
            for n in range(2):
                target = target_group * 2 + n
                sums_send[v, step, n] = held[v, step, n].astype(BF16)
                sums_to(
                    v,
                    step,
                    n,
                    lax.select(through, partner * 2 + core, target),
                    lax.select(through, 2 * groups + target, 2 * own_block + side),
                    lax.select(through, target, kpoints),
                )

    def gather_far(v):
        for step in range(groups - 1):

            @pl.when(step > outward)
            def _(step=step):
                for n in range(2):
                    target = far_target(step) * 2 + n
                    before = sums_slot.at[v, 2 * groups + target]
                    arrival(before, sums_recv_sem.at[v, target]).wait_recv()
                    total = held[v, step, n] + before[...].astype(F32)
                    sums_send[v, step, n] = total.astype(BF16)
                    sums_to(v, step, n, target, 2 * own_block, kpoints)

    def send_own(v):
        totals = screen(v, [sibling, me], whole)
        sending = sums_send.at[v, groups - 1, 0]
        sending[...] = totals[0].astype(BF16)
        slot = 2 * own_block + side
        remote(
            sending,
            sums_slot.at[v, slot],
            sums_send_sem.at[v],
            sums_recv_sem.at[v, kpoints],
            (sibling, band),
        ).start()
        sums_slot[v, slot] = totals[1].astype(BF16)


    def sigma_of(v, peer):
        return jnp.dot(
            vir_turned[aligned(peer * columns, columns), :],
            coupling[v],
            preferred_element_type=F32,
        )

    def make_sigma(v):
        drain(sums_slot.at[v, pl.ds(0, 2 * count + 1)], sums_recv_sem.at[v, kpoints])
        for step in range(count):
            other = lax.rem(pair + step, count)
            for side_core in range(2):
                which = 2 * other + side_core
                total = sums_slot[v, 2 * which].astype(F32)
                if not step:
                    total += sums_slot[v, 2 * which + 1].astype(F32)
                lines = aligned(which * block, block)
                direct = 2.0 * potential[lines, v : v + 1] * occ[lines, :].astype(F32)
                coupling[v, lines, :] = (direct - total).astype(BF16)
        for way, peer in enumerate(others):
            sigma_send[v, way] = sigma_of(v, peer).astype(BF16)
            remote(
                sigma_send.at[v, way],
                sigma_recv.at[v, way],
                sigma_sem.at[vectors],
                sigma_sem.at[v],
                (me, peer),
            ).start()
        out[v] = gaps[...] * trial[v] + sigma_of(v, band)

    take_halves(0)
    for position in range(groups // 2):
        take_corner(position)
    drain(occ_tile.at[pl.ds(0, groups), pl.ds(0, width - piece)], occ_pass_sem.at[1])
    make_pairs(0, (band, near_x, near_y))
    screen_far(0, 0, early)
    for position in range(groups // 2, groups):
        take_corner(position)
    drain(occ_tile.at[pl.ds(0, groups), pl.ds(0, piece)], occ_pass_sem.at[2])
    make_pairs(0, (corner,))
    screen_far(0, 0, late, True)
    send_far(0, 0)
    for step in range(1, groups - 1):
        screen_far(0, step, whole)
        send_far(0, step)
    sum_density()
    for v in range(1, vectors):
        take_halves(v)
        make_pairs(v, (band, near_x, near_y, corner))
        for step in range(groups - 1):
            screen_far(v, step, whole)
            send_far(v, step)
        gather_far(v - 1)
    send_own(0)
    make_potential()
    gather_far(vectors - 1)
    make_sigma(0)
    for v in range(1, vectors):
        send_own(v)
        make_sigma(v)
    for v in range(vectors):
        drain(sigma_recv.at[v], sigma_sem.at[v])
        result = out[v]
        for way in range(bands - 1):
            result += sigma_recv[v, way].astype(F32)
        out[v] = result

    drain(sigma_send, trial_sem.at[vectors])
    drain(sigma_send, sigma_sem.at[vectors])
    for copy in point_copies:
        copy.wait_send()
    drain(occ_tile.at[pl.ds(0, groups), pl.ds(0, width - piece)], occ_send_sem.at[0])
    drain(occ_tile.at[pl.ds(0, groups)], occ_pass_sem.at[0])
    drain(half_all.at[pl.ds(0, groups + 1)], half_send_sem.at[0])
    drain(dens_all.at[pl.ds(0, kpoints - 1)], dens_sem.at[0])
    drain(dens_band.at[pl.ds(0, bands - 1)], dens_band_sem.at[0])
    for v in range(vectors):
        drain(sums_slot.at[v, pl.ds(0, 2 * groups - 1)], sums_send_sem.at[v])
        for far in range(groups - 2):
            for owner_core in range(2):
                pl.when(passing(far_groups[far]))(half_pass(v, far, owner_core).wait_send)


def coupled_part(
    kpoints, bands, occ, vir, trial, occ_energy, vir_energy, coulomb, exch, table
):
    rows, occupied = occ.shape
    vectors, columns = trial.shape[:2]
    groups = kpoints // 2
    block = rows // groups
    width = bands * rows // 2
    vmem = pl.BlockSpec(memory_space=pltpu.VMEM)
    hbm = pl.BlockSpec(memory_space=pltpu.HBM)
    dma = pltpu.SemaphoreType.DMA
    return pl.pallas_call(
        functools.partial(kernel, kpoints, bands, vectors),
        out_shape=jax.ShapeDtypeStruct(trial.shape, F32),
        in_specs=[hbm] * 8,
        out_specs=vmem,
        scratch_shapes=[
            pltpu.VMEM(occ.shape, BF16),
            pltpu.VMEM(vir.shape, BF16),
            pltpu.VMEM(trial.shape, F32),
            pltpu.VMEM(occ_energy.shape, F32),
            pltpu.VMEM(vir_energy.shape, F32),
            pltpu.SMEM(table.shape, jnp.int32),
            pltpu.VMEM((columns, occupied), F32),
            pltpu.VMEM((kpoints, block, width), F32),
            pltpu.VMEM((vectors, bands * columns, occupied), BF16),
            pltpu.VMEM((bands * columns, rows), BF16),
            pltpu.VMEM((vectors, rows, occupied), BF16),
            pltpu.VMEM((kpoints, vectors * block, occupied), BF16),
            pltpu.VMEM((kpoints, width, occupied), BF16),
            pltpu.VMEM((kpoints, vectors, rows), F32),
            pltpu.VMEM((bands, vectors, rows), F32),
            pltpu.VMEM((rows, 128), F32),
            pltpu.VMEM(coulomb.shape, BF16),
            pltpu.VMEM((kpoints, block, width), BF16),
            pltpu.VMEM((kpoints, vectors * block, width), F32),
            pltpu.VMEM((vectors, groups - 1, 2, block, occupied), F32),
            pltpu.VMEM((vectors, groups, 2, block, occupied), BF16),
            pltpu.VMEM((vectors, 2 * groups + kpoints, block, occupied), BF16),
            pltpu.VMEM((vectors, rows, occupied), BF16),
            pltpu.VMEM((vectors, bands - 1, columns, occupied), BF16),
            pltpu.VMEM((vectors, bands - 1, columns, occupied), BF16),
            dma((8,)),
            dma((vectors + 1,)),
            dma((2, groups)),
            dma((1,)),
            dma((groups, bands - 1)),
            dma((3,)),
            dma((1,)),
            dma((vectors, kpoints)),
            dma((vectors, groups - 2, 2)),
            dma((2,)),
            dma((2,)),
            dma((vectors,)),
            dma((vectors, kpoints + 1)),
            dma((vectors + 1,)),
        ],
        compiler_params=pltpu.CompilerParams(
            collective_id=0, has_side_effects=True, vmem_limit_bytes=56 * 2**20
        ),
        name="coupled",
    )(occ, vir, trial, occ_energy, vir_energy, coulomb, exch, table)


def per_device(
    occ_rows, vir_rows, trial_vectors, occ_energy, vir_energy, coulomb, exch_kernel, minus_table
):
    kpoints = lax.axis_size("ka")
    bands = lax.axis_size("band")
    trial_turned = jnp.swapaxes(trial_vectors[0], 1, 2)
    coupled = coupled_part(
        kpoints,
        bands,
        occ_rows[0],
        vir_rows[0],
        trial_turned,
        occ_energy,
        vir_energy,
        coulomb,
        exch_kernel,
        minus_table,
    )
    return jnp.swapaxes(coupled, 1, 2)[None]


def solution(mesh):
    in_specs = (
        P("ka", "band", None),
        P("ka", "band", None),
        P("ka", None, None, "band"),
        P("ka", None),
        P("ka", "band"),
        P("band", None),
        P(None, "band", None),
        P(),
    )
    out_specs = P("ka", None, None, "band")
    return jax.shard_map(
        per_device, mesh=mesh, in_specs=in_specs, out_specs=out_specs, check_vma=False
    )
```

```python
import functools

import jax
import jax.numpy as jnp
from jax import lax
from jax.experimental import pallas as pl
from jax.experimental.pallas import tpu as pltpu
from jax.sharding import PartitionSpec as P

F32 = jnp.float32
BF16 = jnp.bfloat16
CHUNK = 16
SPAN = 512


def dot_nt(left, right, **options):
    return lax.dot_general(
        left, right, (((1,), (1,)), ((), ())), preferred_element_type=F32, **options
    )


def aligned(start, size):
    return pl.ds(pl.multiple_of(start, size), size)


def kernel(
    kpoints,
    bands,
    vectors,
    occ_given,
    vir_given,
    trial_given,
    occ_energy_given,
    vir_energy_given,
    coulomb,
    exch,
    table_given,
    out,
    occ,
    vir,
    trial,
    occ_energy,
    vir_energy,
    table,
    gaps,
    exch_wide,
    trial_full,
    vir_turned,
    half_own,
    half_all,
    occ_tile,
    dens_all,
    dens_band,
    potential,
    coulomb_here,
    exch_tile,
    pairs,
    held,
    sums_send,
    sums_slot,
    coupling,
    sigma_own,
    sigma_send,
    sigma_recv,
    local_sem,
    trial_sem,
    point_sem,
    occ_send_sem,
    occ_sem,
    occ_pass_sem,
    half_send_sem,
    half_recv_sem,
    half_pass_sem,
    half_direct_sem,
    dens_sem,
    dens_band_sem,
    sums_send_sem,
    sums_recv_sem,
    sigma_sem,
):
    me = lax.axis_index("ka")
    band = lax.axis_index("band")
    groups = kpoints // 2
    count = groups // 2
    group = lax.div(me, 2)
    core = lax.rem(me, 2)
    sibling = me + 1 - 2 * core
    pair = lax.div(group, 2)
    side = lax.rem(group, 2)
    partner = group + 1 - 2 * side
    rows, occupied = occ.shape
    columns = trial.shape[1]
    block = rows // groups
    piece = rows // 2
    width = bands * piece
    near_x = band + 1 - 2 * lax.rem(band, 2)
    near_y = lax.rem(band + 2, bands)
    corner = bands - 1 - band
    others = (corner, near_x, near_y)

    def tile_of(k):
        return lax.rem(k, 2) * groups + lax.div(k, 2)

    def remote(source, target, send, recv, device):
        return pltpu.make_async_remote_copy(
            src_ref=source,
            dst_ref=target,
            send_sem=send,
            recv_sem=recv,
            device_id=device,
            device_id_type=pl.DeviceIdType.MESH,
        )

    def arrival(target, recv):
        return remote(target, target, recv, recv, (sibling, band))

    def drain(held, sem):
        pltpu.make_async_copy(held, held, sem).wait()

    barrier = pltpu.get_barrier_semaphore()
    for peer in others:
        pl.semaphore_signal(
            barrier, inc=1, device_id=(me, peer), device_id_type=pl.DeviceIdType.MESH
        )
    for step in range(1, kpoints):
        pl.semaphore_signal(
            barrier,
            inc=1,
            device_id=(lax.rem(me + step, kpoints), band),
            device_id_type=pl.DeviceIdType.MESH,
        )

    load_copies = []
    for given, here in (
        (trial_given, trial),
        (occ_given, occ),
        (vir_given, vir),
        (table_given, table),
        (occ_energy_given, occ_energy),
        (vir_energy_given, vir_energy),
    ):
        copy = pltpu.make_async_copy(given, here, local_sem.at[2 + len(load_copies)])
        copy.start()
        load_copies.append(copy)
    trial_load, occ_load, vir_load, *other_loads = load_copies
    for part in range(bands):
        pltpu.make_async_copy(
            exch.at[
                :,
                aligned((2 * pair + core) * block, block),
                aligned(part * rows + side * piece, piece),
            ],
            exch_tile.at[:, :, pl.ds(part * piece, piece)],
            local_sem.at[1],
        ).start()
    coulomb_copy = pltpu.make_async_copy(coulomb, coulomb_here, local_sem.at[0])
    coulomb_copy.start()

    own_columns = aligned(band * columns, columns)
    trial_load.wait()
    trial_full[:, own_columns, :] = trial[...].astype(BF16)
    pl.semaphore_wait(barrier, len(others) + kpoints - 1)

    for v in range(vectors):
        for peer in others:
            remote(
                trial_full.at[v, own_columns],
                trial_full.at[v, own_columns],
                trial_sem.at[vectors],
                trial_sem.at[v],
                (me, peer),
            ).start()

    def piece_of(owner):
        return aligned(owner * piece, piece)

    far_groups = []
    for step in range(groups - 2):
        low = lax.rem(2 * pair + 2 + step, groups)
        high = lax.rem(2 * pair + 2 * groups - 1 - step, groups)
        far_groups.append(lax.select(2 * pair < count, low, high))
    far_groups.reverse()
    order = [group, partner] + far_groups

    mine = tile_of(me)
    occ_load.wait()
    point_copies = []
    for step, peer in enumerate(order[1:]):
        copy = remote(
            occ.at[aligned(lax.rem(peer, 2) * piece, piece)],
            occ_tile.at[mine, piece_of(band)],
            point_sem.at[0, step],
            point_sem.at[1, group],
            (peer * 2 + core, band),
        )
        copy.start()
        point_copies.append(copy)
    occ_tile[mine, piece_of(band), :] = occ[aligned(side * piece, piece), :]

    def occ_out(source_group):
        tile = core * groups + source_group
        here = occ_tile.at[tile, piece_of(band)]
        for way, peer in ((1, near_x), (2, near_y)):
            remote(
                here,
                here,
                occ_send_sem.at[0],
                occ_sem.at[source_group, way - 1],
                (me, peer),
            ).start()
        occ_pass(source_group, 0, band).start()

    def occ_pass(source_group, way, owner):
        here = occ_tile.at[core * groups + source_group, piece_of(owner)]
        return remote(
            here,
            here,
            occ_pass_sem.at[0],
            occ_pass_sem.at[1 + way // (bands - 1)],
            (sibling, band),
        )

    occ_out(group)
    vir_load.wait()
    vir_turned[...] = vir[...].T
    for copy in other_loads:
        copy.wait()
    turned = jnp.broadcast_to(vir_energy[...], (occupied, columns)).T
    gaps[...] = turned - occ_energy[...]
    drain(exch_tile, local_sem.at[1])

    def widen(k, carry):
        exch_wide[k] = exch_tile[k].astype(F32)
        return carry

    lax.fori_loop(0, kpoints, widen, 0)

    def take_point(source_group):
        arrival(
            occ_tile.at[core * groups + source_group, piece_of(band)],
            point_sem.at[1, source_group],
        ).wait_recv()
        occ_out(source_group)

    def own_half(v):
        drain(sigma_recv.at[v], trial_sem.at[v])
        half_own[v] = jnp.dot(vir[...], trial_full[v], preferred_element_type=F32).astype(BF16)
        lines = pl.ds(v * block, block)
        own_block = 2 * pair + core
        half_all[me, lines, :] = half_own[v, aligned(own_block * block, block), :]
        destinations = []
        for step in range(1, count):
            other = lax.rem(pair + step, count)
            near = lax.select(other > pair, 2 * other, 2 * other + 1)
            destinations += [(2 * other + side_core, near * 2 + side_core) for side_core in range(2)]
        destinations += [(2 * pair + side_core, partner * 2 + side_core) for side_core in range(2)]
        destinations.append((2 * pair + 1 - core, sibling))
        for which, device in destinations:
            remote(
                half_own.at[v, aligned(which * block, block)],
                half_all.at[me, lines],
                half_send_sem.at[0],
                half_recv_sem.at[v, me],
                (device, band),
            ).start()
        if v == 0:
            for copy, direct in direct_copies():
                pl.when(direct)(copy.start)

    def direct_copies():
        copies = []
        for step in range(1, count):
            other = lax.rem(pair + step, count)
            above = other > pair
            distant = lax.select(above, 2 * other + 1, 2 * other)
            for side_core in range(2):
                copy = remote(
                    half_own.at[0, aligned((2 * other + side_core) * block, block)],
                    half_all.at[me, pl.ds(0, block)],
                    half_direct_sem.at[step - 1, side_core],
                    half_recv_sem.at[0, me],
                    (distant * 2 + side_core, band),
                )
                copies.append((copy, lax.select(above, side, 1 - side) == 1))
        return copies

    def half_pass(v, position, owner_core):
        source = far_groups[position] * 2 + owner_core
        here = half_all.at[source, pl.ds(v * block, block)]
        return remote(
            here,
            here,
            half_pass_sem.at[v, position, owner_core],
            half_recv_sem.at[v, source],
            (partner * 2 + core, band),
        )

    def take_half(v, source):
        here = half_all.at[source, pl.ds(v * block, block)]
        arrival(here, half_recv_sem.at[v, source]).wait_recv()

    def passing(v, source_group):
        below = source_group < 2 * pair
        near = lax.select(below, 1 - side, side)
        if v:
            return near == 1
        source_side = lax.rem(source_group, 2)
        return near * lax.select(below, 1 - source_side, source_side) == 1

    def take_far(v, position):
        for owner_core in range(2):
            take_half(v, far_groups[position] * 2 + owner_core)
            pl.when(passing(v, far_groups[position]))(half_pass(v, position, owner_core).start)

    def occ_turn(position):
        source_group = order[position]
        tile = core * groups + source_group
        if position < groups // 2:
            owner, onward = near_x, near_y
        else:
            owner, onward = near_y, near_x
        here = occ_tile.at[tile, piece_of(owner)]
        return remote(
            here,
            here,
            occ_send_sem.at[0],
            occ_sem.at[source_group, 2],
            (me, onward),
        )

    def occ_in(position):
        source_group = order[position]
        tile = core * groups + source_group
        for way, owner in ((1, near_x), (2, near_y)):
            here = occ_tile.at[tile, piece_of(owner)]
            arrival(here, occ_sem.at[source_group, way - 1]).wait_recv()
            if (position < groups // 2) == (way == 1):
                occ_turn(position).start()
            occ_pass(source_group, way, owner).start()

    inner = lax.select(2 * pair < count, side, 1 - side) == 1

    take_point(partner)
    for v in range(vectors):
        own_half(v)
        for source_group in far_groups[v::vectors]:
            take_point(source_group)
    for position in range(groups):
        occ_in(position)
        if position < groups - 2:

            @pl.when(inner)
            def _(far=position):
                take_far(0, far)

    @pl.when(inner)
    def _():
        for v in range(1, vectors):
            for far in range(groups - 2):
                take_far(v, far)

    ones = jnp.ones((8, occupied), F32)
    occ_wide = occ[...].astype(F32)
    dens_all[me] = jnp.concatenate(
        [
            dot_nt(ones, occ_wide * half_own[v].astype(F32), precision=lax.Precision.HIGHEST)[:1]
            for v in range(vectors)
        ],
        axis=0,
    )
    for step in range(1, kpoints):
        remote(
            dens_all.at[me],
            dens_all.at[me],
            dens_sem.at[0],
            dens_sem.at[1],
            (lax.rem(me + step, kpoints), band),
        ).start()

    def take_corner(position):
        source_group = order[position]
        here = occ_tile.at[core * groups + source_group, piece_of(corner)]
        arrival(here, occ_sem.at[source_group, 2]).wait_recv()
        occ_pass(source_group, bands - 1, corner).start()

    def take_halves(v):
        take_half(v, sibling)
        for source in (partner * 2, partner * 2 + 1):
            take_half(v, source)

        @pl.when(jnp.logical_not(inner))
        def _():
            for far in range(groups - 2):
                take_far(v, far)

    def make_pairs(v, owners):
        lines = pl.ds(v * block, block)
        for source in range(kpoints):
            tile = tile_of(source)
            if len(owners) == bands:
                pairs[source, lines] = dot_nt(half_all[source, lines], occ_tile[tile])
                continue
            for owner in owners:
                part = piece_of(owner)
                pairs[source, lines, part] = dot_nt(
                    half_all[source, lines], occ_tile[tile, part]
                )

    def sum_density():
        drain(dens_all.at[pl.ds(0, kpoints - 1)], dens_sem.at[1])
        density = dens_all[0]
        for k in range(1, kpoints):
            density += dens_all[k]
        dens_band[band] = density
        for peer in others:
            remote(
                dens_band.at[band],
                dens_band.at[band],
                dens_band_sem.at[0],
                dens_band_sem.at[1],
                (me, peer),
            ).start()

    def make_potential():
        drain(dens_band.at[pl.ds(0, bands - 1)], dens_band_sem.at[1])
        coulomb_copy.wait()
        spread = jnp.zeros((16 - vectors, rows), F32)
        total = jnp.zeros((rows, 16), F32)
        for part in range(bands):
            here = jnp.concatenate([dens_band[part], spread], axis=0).astype(BF16)
            total += dot_nt(coulomb_here[:, part * rows : (part + 1) * rows], here)
        potential[:, :16] = total

    def screen(v, targets, spans):
        sources = [[table[target, q] for q in range(kpoints)] for target in targets]
        results = [jnp.zeros((block, occupied), F32) for _ in targets]
        for across, span in spans:
            chunks = [[] for _ in targets]
            for start in range(0, block, CHUNK):
                totals = [jnp.zeros((CHUNK, span), F32) for _ in targets]
                for q in range(kpoints):
                    factor = exch_wide[q, pl.ds(start, CHUNK), across]
                    for n in range(len(targets)):
                        there = pl.ds(v * block + start, CHUNK)
                        totals[n] += pairs[sources[n][q], there, across] * factor
                for n in range(len(targets)):
                    chunks[n].append(totals[n].astype(BF16))
            for n, target in enumerate(targets):
                results[n] += jnp.dot(
                    jnp.concatenate(chunks[n], axis=0),
                    occ_tile[tile_of(target), across],
                    preferred_element_type=F32,
                )
        return results

    whole = [(pl.ds(first, SPAN), SPAN) for first in range(0, width, SPAN)]
    early = [(piece_of(owner), piece) for owner in (band, near_x, near_y)]
    late = [(piece_of(corner), piece)]

    own_block = 2 * pair + core
    lower = 2 * pair
    higher = groups - 2 - lower
    outward = lax.select(side == 0, higher, lower)

    def far_target(step):
        rising = lax.select(step <= higher, groups - 1 - step, step - higher - 1)
        falling = lax.select(step <= lower, step, groups + lower - step)
        return lax.select(side == 0, rising, falling)

    def sums_to(v, step, n, device, slot, recv):
        remote(
            sums_send.at[v, step, n],
            sums_slot.at[v, slot],
            sums_send_sem.at[v],
            sums_recv_sem.at[v, recv],
            (device, band),
        ).start()

    def screen_far(v, step, spans, before=None):
        target_group = far_target(step)
        totals = screen(v, [target_group * 2 + n for n in range(2)], spans)
        for n in range(2):
            held[v, step, n] = totals[n] if before is None else held[v, step, n] + totals[n]

    def send_far(v, step):
        target_group = far_target(step)
        through = step < outward

        @pl.when(step <= outward)
        def _():
            for n in range(2):
                target = target_group * 2 + n
                sums_send[v, step, n] = held[v, step, n].astype(BF16)
                sums_to(
                    v,
                    step,
                    n,
                    lax.select(through, partner * 2 + core, target),
                    lax.select(through, 2 * groups + target, 2 * own_block + side),
                    lax.select(through, target, kpoints),
                )

    def gather_far(v):
        for step in range(groups - 1):

            @pl.when(step > outward)
            def _(step=step):
                for n in range(2):
                    target = far_target(step) * 2 + n
                    before = sums_slot.at[v, 2 * groups + target]
                    arrival(before, sums_recv_sem.at[v, target]).wait_recv()
                    total = held[v, step, n] + before[...].astype(F32)
                    sums_send[v, step, n] = total.astype(BF16)
                    sums_to(v, step, n, target, 2 * own_block, kpoints)

    def send_own(v):
        totals = screen(v, [sibling, me], whole)
        sending = sums_send.at[v, groups - 1, 0]
        sending[...] = totals[0].astype(BF16)
        slot = 2 * own_block + side
        remote(
            sending,
            sums_slot.at[v, slot],
            sums_send_sem.at[v],
            sums_recv_sem.at[v, kpoints],
            (sibling, band),
        ).start()
        sums_slot[v, slot] = totals[1].astype(BF16)


    def make_sigma(v):
        drain(sums_slot.at[v, pl.ds(0, 2 * count + 1)], sums_recv_sem.at[v, kpoints])
        for step in range(count):
            other = lax.rem(pair + step, count)
            for side_core in range(2):
                which = 2 * other + side_core
                total = sums_slot[v, 2 * which].astype(F32)
                if not step:
                    total += sums_slot[v, 2 * which + 1].astype(F32)
                lines = aligned(which * block, block)
                direct = 2.0 * potential[lines, v : v + 1] * occ[lines, :].astype(F32)
                coupling[v, lines, :] = (direct - total).astype(BF16)
        total = jnp.dot(vir_turned[...], coupling[v], preferred_element_type=F32)
        sigma_own[...] = total
        sigma_send[v] = total.astype(BF16)
        for way, peer in enumerate(others):
            remote(
                sigma_send.at[v, pl.ds(pl.multiple_of(peer * columns, 16), columns)],
                sigma_recv.at[v, way],
                sigma_sem.at[vectors],
                sigma_sem.at[v],
                (me, peer),
            ).start()
        out[v] = gaps[...] * trial[v] + sigma_own[pl.ds(pl.multiple_of(band * columns, 16), columns)]

    take_halves(0)
    drain(occ_tile.at[pl.ds(0, groups), pl.ds(0, width - piece)], occ_pass_sem.at[1])
    make_pairs(0, (band, near_x, near_y))
    for step in range(groups - 2):
        take_corner(step)
        screen_far(0, step, early)
    for position in range(groups - 2, groups):
        take_corner(position)
    drain(occ_tile.at[pl.ds(0, groups), pl.ds(0, piece)], occ_pass_sem.at[2])
    make_pairs(0, (corner,))
    for step in range(groups - 2):
        screen_far(0, step, late, True)
        send_far(0, step)

    def both_far(v, step):
        screen_far(v, step, whole)
        send_far(v, step)

    sum_density()
    for v in range(1, vectors):
        take_halves(v)
        make_pairs(v, (band, near_x, near_y, corner))
        for step in range(groups - 2):
            both_far(v, step)
    for v in range(vectors):
        both_far(v, groups - 2)
        if v == 0:
            gather_far(0)
    send_own(0)
    for v in range(1, vectors):
        gather_far(v)
        send_own(v)
    make_potential()
    for v in range(vectors):
        make_sigma(v)
    for v in range(vectors):
        drain(sigma_recv.at[v], sigma_sem.at[v])
        result = out[v]
        for way in range(bands - 1):
            result += sigma_recv[v, way].astype(F32)
        out[v] = result

    drain(sigma_recv, trial_sem.at[vectors])
    drain(sigma_recv, sigma_sem.at[vectors])
    for copy in point_copies:
        copy.wait_send()
    drain(occ_tile.at[pl.ds(0, groups), pl.ds(0, width - piece)], occ_send_sem.at[0])
    drain(occ_tile.at[pl.ds(0, groups)], occ_pass_sem.at[0])
    drain(half_all.at[pl.ds(0, groups + 1)], half_send_sem.at[0])
    drain(dens_all.at[pl.ds(0, kpoints - 1)], dens_sem.at[0])
    drain(dens_band.at[pl.ds(0, bands - 1)], dens_band_sem.at[0])
    for v in range(vectors):
        drain(sums_slot.at[v, pl.ds(0, 2 * groups - 1)], sums_send_sem.at[v])
        for far in range(groups - 2):
            for owner_core in range(2):
                pl.when(passing(v, far_groups[far]))(half_pass(v, far, owner_core).wait_send)
    for copy, direct in direct_copies():
        pl.when(direct)(copy.wait_send)


def coupled_part(
    kpoints, bands, occ, vir, trial, occ_energy, vir_energy, coulomb, exch, table
):
    rows, occupied = occ.shape
    vectors, columns = trial.shape[:2]
    groups = kpoints // 2
    count = groups // 2
    block = rows // groups
    width = bands * rows // 2
    vmem = pl.BlockSpec(memory_space=pltpu.VMEM)
    hbm = pl.BlockSpec(memory_space=pltpu.HBM)
    dma = pltpu.SemaphoreType.DMA
    return pl.pallas_call(
        functools.partial(kernel, kpoints, bands, vectors),
        out_shape=pltpu.VMEM(trial.shape, F32),
        in_specs=[hbm] * 8,
        out_specs=vmem,
        scratch_shapes=[
            pltpu.VMEM(occ.shape, BF16),
            pltpu.VMEM(vir.shape, BF16),
            pltpu.VMEM(trial.shape, F32),
            pltpu.VMEM(occ_energy.shape, F32),
            pltpu.VMEM(vir_energy.shape, F32),
            pltpu.SMEM(table.shape, jnp.int32),
            pltpu.VMEM((columns, occupied), F32),
            pltpu.VMEM((kpoints, block, width), F32),
            pltpu.VMEM((vectors, bands * columns, occupied), BF16),
            pltpu.VMEM((bands * columns, rows), BF16),
            pltpu.VMEM((vectors, rows, occupied), BF16),
            pltpu.VMEM((kpoints, vectors * block, occupied), BF16),
            pltpu.VMEM((kpoints, width, occupied), BF16),
            pltpu.VMEM((kpoints, vectors, rows), F32),
            pltpu.VMEM((bands, vectors, rows), F32),
            pltpu.VMEM((rows, 128), F32),
            pltpu.VMEM(coulomb.shape, BF16),
            pltpu.VMEM((kpoints, block, width), BF16),
            pltpu.VMEM((kpoints, vectors * block, width), F32),
            pltpu.VMEM((vectors, groups - 1, 2, block, occupied), F32),
            pltpu.VMEM((vectors, groups, 2, block, occupied), BF16),
            pltpu.VMEM((vectors, 2 * groups + kpoints, block, occupied), BF16),
            pltpu.VMEM((vectors, rows, occupied), BF16),
            pltpu.VMEM((bands * columns, occupied), F32),
            pltpu.VMEM((vectors, bands * columns, occupied), BF16),
            pltpu.VMEM((vectors, bands - 1, columns, occupied), BF16),
            dma((8,)),
            dma((vectors + 1,)),
            dma((2, groups)),
            dma((1,)),
            dma((groups, bands - 1)),
            dma((3,)),
            dma((1,)),
            dma((vectors, kpoints)),
            dma((vectors, groups - 2, 2)),
            dma((count - 1, 2)),
            dma((2,)),
            dma((2,)),
            dma((vectors,)),
            dma((vectors, kpoints + 1)),
            dma((vectors + 1,)),
        ],
        compiler_params=pltpu.CompilerParams(
            collective_id=0, has_side_effects=True, vmem_limit_bytes=40 * 2**20
        ),
        name="coupled",
    )(
        *(
            pltpu.with_memory_space_constraint(given, pltpu.HBM)
            for given in (occ, vir, trial, occ_energy, vir_energy, coulomb, exch, table)
        )
    )


def per_device(
    occ_rows, vir_rows, trial_vectors, occ_energy, vir_energy, coulomb, exch_kernel, minus_table
):
    kpoints = lax.axis_size("ka")
    bands = lax.axis_size("band")
    trial_turned = jnp.swapaxes(trial_vectors[0], 1, 2)
    coupled = coupled_part(
        kpoints,
        bands,
        occ_rows[0],
        vir_rows[0],
        trial_turned,
        occ_energy,
        vir_energy,
        coulomb,
        exch_kernel,
        minus_table,
    )
    return jnp.swapaxes(coupled, 1, 2)[None]


def solution(mesh):
    in_specs = (
        P("ka", "band", None),
        P("ka", "band", None),
        P("ka", None, None, "band"),
        P("ka", None),
        P("ka", "band"),
        P("band", None),
        P(None, "band", None),
        P(),
    )
    out_specs = P("ka", None, None, "band")
    return jax.shard_map(
        per_device, mesh=mesh, in_specs=in_specs, out_specs=out_specs, check_vma=False
    )
```

```python
import functools

import jax
import jax.numpy as jnp
from jax import lax
from jax.experimental import pallas as pl
from jax.experimental.pallas import tpu as pltpu
from jax.sharding import PartitionSpec as P

F32 = jnp.float32
BF16 = jnp.bfloat16
CHUNK = 16
SPAN = 512


def dot_nt(left, right, **options):
    return lax.dot_general(
        left, right, (((1,), (1,)), ((), ())), preferred_element_type=F32, **options
    )


def aligned(start, size):
    return pl.ds(pl.multiple_of(start, size), size)


def kernel(
    kpoints,
    bands,
    vectors,
    occ_given,
    vir_given,
    trial_given,
    occ_energy_given,
    vir_energy_given,
    coulomb,
    exch,
    table_given,
    out,
    occ,
    vir,
    trial,
    occ_energy,
    vir_energy,
    table,
    gaps,
    exch_wide,
    trial_full,
    vir_turned,
    half_own,
    half_all,
    occ_tile,
    dens_all,
    dens_band,
    potential,
    coulomb_here,
    exch_tile,
    pairs,
    held,
    sums_send,
    sums_slot,
    coupling,
    sigma_own,
    sigma_send,
    sigma_recv,
    local_sem,
    trial_sem,
    point_sem,
    occ_send_sem,
    occ_sem,
    occ_pass_sem,
    half_send_sem,
    half_recv_sem,
    half_pass_sem,
    half_direct_sem,
    dens_sem,
    dens_band_sem,
    sums_send_sem,
    sums_recv_sem,
    sigma_sem,
):
    me = lax.axis_index("ka")
    band = lax.axis_index("band")
    groups = kpoints // 2
    count = groups // 2
    group = lax.div(me, 2)
    core = lax.rem(me, 2)
    sibling = me + 1 - 2 * core
    pair = lax.div(group, 2)
    side = lax.rem(group, 2)
    partner = group + 1 - 2 * side
    rows, occupied = occ.shape
    columns = trial.shape[1]
    block = rows // groups
    piece = rows // 2
    width = bands * piece
    near_x = band + 1 - 2 * lax.rem(band, 2)
    near_y = lax.rem(band + 2, bands)
    corner = bands - 1 - band
    others = (corner, near_x, near_y)

    def tile_of(k):
        return lax.rem(k, 2) * groups + lax.div(k, 2)

    def remote(source, target, send, recv, device):
        return pltpu.make_async_remote_copy(
            src_ref=source,
            dst_ref=target,
            send_sem=send,
            recv_sem=recv,
            device_id=device,
            device_id_type=pl.DeviceIdType.MESH,
        )

    def arrival(target, recv):
        return remote(target, target, recv, recv, (sibling, band))

    def drain(held, sem):
        pltpu.make_async_copy(held, held, sem).wait()

    barrier = pltpu.get_barrier_semaphore()
    for peer in others:
        pl.semaphore_signal(
            barrier, inc=1, device_id=(me, peer), device_id_type=pl.DeviceIdType.MESH
        )
    for step in range(1, kpoints):
        pl.semaphore_signal(
            barrier,
            inc=1,
            device_id=(lax.rem(me + step, kpoints), band),
            device_id_type=pl.DeviceIdType.MESH,
        )

    load_copies = []
    for given, here in (
        (trial_given, trial),
        (occ_given, occ),
        (vir_given, vir),
        (table_given, table),
        (occ_energy_given, occ_energy),
        (vir_energy_given, vir_energy),
    ):
        copy = pltpu.make_async_copy(given, here, local_sem.at[2 + len(load_copies)])
        copy.start()
        load_copies.append(copy)
    trial_load, occ_load, vir_load, *other_loads = load_copies
    for part in range(bands):
        pltpu.make_async_copy(
            exch.at[
                :,
                aligned((2 * pair + core) * block, block),
                aligned(part * rows + side * piece, piece),
            ],
            exch_tile.at[:, :, pl.ds(part * piece, piece)],
            local_sem.at[1],
        ).start()
    coulomb_copy = pltpu.make_async_copy(coulomb, coulomb_here, local_sem.at[0])
    coulomb_copy.start()

    own_columns = aligned(band * columns, columns)
    trial_load.wait()
    trial_full[:, own_columns, :] = trial[...].astype(BF16)
    pl.semaphore_wait(barrier, len(others) + kpoints - 1)

    for v in range(vectors):
        for peer in others:
            remote(
                trial_full.at[v, own_columns],
                trial_full.at[v, own_columns],
                trial_sem.at[vectors],
                trial_sem.at[v],
                (me, peer),
            ).start()

    def piece_of(owner):
        return aligned(owner * piece, piece)

    far_groups = []
    for step in range(groups - 2):
        low = lax.rem(2 * pair + 2 + step, groups)
        high = lax.rem(2 * pair + 2 * groups - 1 - step, groups)
        far_groups.append(lax.select(2 * pair < count, low, high))
    far_groups.reverse()
    order = [group, partner] + far_groups

    mine = tile_of(me)
    occ_load.wait()
    point_copies = []
    for step, peer in enumerate(order[1:]):
        copy = remote(
            occ.at[aligned(lax.rem(peer, 2) * piece, piece)],
            occ_tile.at[mine, piece_of(band)],
            point_sem.at[0, step],
            point_sem.at[1, group],
            (peer * 2 + core, band),
        )
        copy.start()
        point_copies.append(copy)
    occ_tile[mine, piece_of(band), :] = occ[aligned(side * piece, piece), :]

    def occ_out(source_group):
        tile = core * groups + source_group
        here = occ_tile.at[tile, piece_of(band)]
        for way, peer in ((1, near_x), (2, near_y)):
            remote(
                here,
                here,
                occ_send_sem.at[0],
                occ_sem.at[source_group, way - 1],
                (me, peer),
            ).start()
        occ_pass(source_group, 0, band).start()

    def occ_pass(source_group, way, owner):
        here = occ_tile.at[core * groups + source_group, piece_of(owner)]
        return remote(
            here,
            here,
            occ_pass_sem.at[0],
            occ_pass_sem.at[1 + way // (bands - 1)],
            (sibling, band),
        )

    occ_out(group)
    vir_load.wait()
    vir_turned[...] = vir[...].T
    for copy in other_loads:
        copy.wait()
    turned = jnp.broadcast_to(vir_energy[...], (occupied, columns)).T
    gaps[...] = turned - occ_energy[...]
    drain(exch_tile, local_sem.at[1])

    def widen(k, carry):
        exch_wide[k] = exch_tile[k].astype(F32)
        return carry

    lax.fori_loop(0, kpoints, widen, 0)

    def take_point(source_group):
        arrival(
            occ_tile.at[core * groups + source_group, piece_of(band)],
            point_sem.at[1, source_group],
        ).wait_recv()
        occ_out(source_group)

    def own_half(v):
        drain(sigma_recv.at[v], trial_sem.at[v])
        half_own[v] = jnp.dot(vir[...], trial_full[v], preferred_element_type=F32).astype(BF16)
        lines = pl.ds(v * block, block)
        own_block = 2 * pair + core
        half_all[me, lines, :] = half_own[v, aligned(own_block * block, block), :]
        destinations = []
        for step in range(1, count):
            other = lax.rem(pair + step, count)
            near = lax.select(other > pair, 2 * other, 2 * other + 1)
            destinations += [(2 * other + side_core, near * 2 + side_core) for side_core in range(2)]
        destinations += [(2 * pair + side_core, partner * 2 + side_core) for side_core in range(2)]
        destinations.append((2 * pair + 1 - core, sibling))
        for which, device in destinations:
            remote(
                half_own.at[v, aligned(which * block, block)],
                half_all.at[me, lines],
                half_send_sem.at[0],
                half_recv_sem.at[v, me],
                (device, band),
            ).start()
        if v == 0:
            for copy, direct in direct_copies():
                pl.when(direct)(copy.start)

    def direct_copies():
        copies = []
        for step in range(1, count):
            other = lax.rem(pair + step, count)
            above = other > pair
            distant = lax.select(above, 2 * other + 1, 2 * other)
            for side_core in range(2):
                copy = remote(
                    half_own.at[0, aligned((2 * other + side_core) * block, block)],
                    half_all.at[me, pl.ds(0, block)],
                    half_direct_sem.at[step - 1, side_core],
                    half_recv_sem.at[0, me],
                    (distant * 2 + side_core, band),
                )
                copies.append((copy, lax.select(above, side, 1 - side) == 1))
        return copies

    def half_pass(v, position, owner_core):
        source = far_groups[position] * 2 + owner_core
        here = half_all.at[source, pl.ds(v * block, block)]
        return remote(
            here,
            here,
            half_pass_sem.at[v, position, owner_core],
            half_recv_sem.at[v, source],
            (partner * 2 + core, band),
        )

    def take_half(v, source):
        here = half_all.at[source, pl.ds(v * block, block)]
        arrival(here, half_recv_sem.at[v, source]).wait_recv()

    def passing(v, source_group):
        below = source_group < 2 * pair
        near = lax.select(below, 1 - side, side)
        if v:
            return near == 1
        source_side = lax.rem(source_group, 2)
        return near * lax.select(below, 1 - source_side, source_side) == 1

    def take_far(v, position):
        for owner_core in range(2):
            take_half(v, far_groups[position] * 2 + owner_core)
            pl.when(passing(v, far_groups[position]))(half_pass(v, position, owner_core).start)

    def occ_turn(position):
        source_group = order[position]
        tile = core * groups + source_group
        if position < groups // 2:
            owner, onward = near_x, near_y
        else:
            owner, onward = near_y, near_x
        here = occ_tile.at[tile, piece_of(owner)]
        return remote(
            here,
            here,
            occ_send_sem.at[0],
            occ_sem.at[source_group, 2],
            (me, onward),
        )

    def occ_in(position):
        source_group = order[position]
        tile = core * groups + source_group
        for way, owner in ((1, near_x), (2, near_y)):
            here = occ_tile.at[tile, piece_of(owner)]
            arrival(here, occ_sem.at[source_group, way - 1]).wait_recv()
            if (position < groups // 2) == (way == 1):
                occ_turn(position).start()
            occ_pass(source_group, way, owner).start()

    inner = lax.select(2 * pair < count, side, 1 - side) == 1

    take_point(partner)
    for v in range(vectors):
        own_half(v)
        for source_group in far_groups[v::vectors]:
            take_point(source_group)
    for position in range(groups):
        occ_in(position)
        if position < groups - 2:

            @pl.when(inner)
            def _(far=position):
                take_far(0, far)

    ones = jnp.ones((8, occupied), F32)
    occ_wide = occ[...].astype(F32)
    dens_all[me] = jnp.concatenate(
        [
            dot_nt(ones, occ_wide * half_own[v].astype(F32), precision=lax.Precision.HIGHEST)[:1]
            for v in range(vectors)
        ],
        axis=0,
    )
    for step in range(1, kpoints):
        remote(
            dens_all.at[me],
            dens_all.at[me],
            dens_sem.at[0],
            dens_sem.at[1],
            (lax.rem(me + step, kpoints), band),
        ).start()

    @pl.when(inner)
    def _():
        for v in range(1, vectors):
            for far in range(groups - 2):
                take_far(v, far)

    def take_corner(position):
        source_group = order[position]
        here = occ_tile.at[core * groups + source_group, piece_of(corner)]
        arrival(here, occ_sem.at[source_group, 2]).wait_recv()
        occ_pass(source_group, bands - 1, corner).start()

    def take_halves(v):
        take_half(v, sibling)
        for source in (partner * 2, partner * 2 + 1):
            take_half(v, source)

        @pl.when(jnp.logical_not(inner))
        def _():
            for far in range(groups - 2):
                take_far(v, far)

    def make_pairs(v, owners):
        lines = pl.ds(v * block, block)
        for source in range(kpoints):
            tile = tile_of(source)
            if len(owners) == bands:
                pairs[source, lines] = dot_nt(half_all[source, lines], occ_tile[tile])
                continue
            for owner in owners:
                part = piece_of(owner)
                pairs[source, lines, part] = dot_nt(
                    half_all[source, lines], occ_tile[tile, part]
                )

    def sum_density():
        drain(dens_all.at[pl.ds(0, kpoints - 1)], dens_sem.at[1])
        density = dens_all[0]
        for k in range(1, kpoints):
            density += dens_all[k]
        dens_band[band] = density
        for peer in others:
            remote(
                dens_band.at[band],
                dens_band.at[band],
                dens_band_sem.at[0],
                dens_band_sem.at[1],
                (me, peer),
            ).start()

    def make_potential():
        drain(dens_band.at[pl.ds(0, bands - 1)], dens_band_sem.at[1])
        coulomb_copy.wait()
        spread = jnp.zeros((16 - vectors, rows), F32)
        total = jnp.zeros((rows, 16), F32)
        for part in range(bands):
            here = jnp.concatenate([dens_band[part], spread], axis=0).astype(BF16)
            total += dot_nt(coulomb_here[:, part * rows : (part + 1) * rows], here)
        potential[:, :16] = total

    def screen(v, targets, spans):
        sources = [[table[target, q] for q in range(kpoints)] for target in targets]
        results = [jnp.zeros((block, occupied), F32) for _ in targets]
        for across, span in spans:
            chunks = [[] for _ in targets]
            for start in range(0, block, CHUNK):
                totals = [jnp.zeros((CHUNK, span), F32) for _ in targets]
                for q in range(kpoints):
                    factor = exch_wide[q, pl.ds(start, CHUNK), across]
                    for n in range(len(targets)):
                        there = pl.ds(v * block + start, CHUNK)
                        totals[n] += pairs[sources[n][q], there, across] * factor
                for n in range(len(targets)):
                    chunks[n].append(totals[n].astype(BF16))
            for n, target in enumerate(targets):
                results[n] += jnp.dot(
                    jnp.concatenate(chunks[n], axis=0),
                    occ_tile[tile_of(target), across],
                    preferred_element_type=F32,
                )
        return results

    whole = [(pl.ds(first, SPAN), SPAN) for first in range(0, width, SPAN)]
    early = [(piece_of(owner), piece) for owner in (band, near_x, near_y)]
    late = [(piece_of(corner), piece)]

    own_block = 2 * pair + core
    lower = 2 * pair
    higher = groups - 2 - lower
    outward = lax.select(side == 0, higher, lower)

    def far_target(step):
        rising = lax.select(step <= higher, groups - 1 - step, step - higher - 1)
        falling = lax.select(step <= lower, step, groups + lower - step)
        return lax.select(side == 0, rising, falling)

    def sums_to(v, step, n, device, slot, recv):
        remote(
            sums_send.at[v, step, n],
            sums_slot.at[v, slot],
            sums_send_sem.at[v],
            sums_recv_sem.at[v, recv],
            (device, band),
        ).start()

    def screen_far(v, step, spans, before=None):
        target_group = far_target(step)
        totals = screen(v, [target_group * 2 + n for n in range(2)], spans)
        for n in range(2):
            held[v, step, n] = totals[n] if before is None else held[v, step, n] + totals[n]

    def send_far(v, step):
        target_group = far_target(step)
        through = step < outward

        @pl.when(step <= outward)
        def _():
            for n in range(2):
                target = target_group * 2 + n
                sums_send[v, step, n] = held[v, step, n].astype(BF16)
                sums_to(
                    v,
                    step,
                    n,
                    lax.select(through, partner * 2 + core, target),
                    lax.select(through, 2 * groups + target, 2 * own_block + side),
                    lax.select(through, target, kpoints),
                )

    def gather_far(v, step):
        @pl.when(step > outward)
        def _():
            for n in range(2):
                target = far_target(step) * 2 + n
                before = sums_slot.at[v, 2 * groups + target]
                arrival(before, sums_recv_sem.at[v, target]).wait_recv()
                total = held[v, step, n] + before[...].astype(F32)
                sums_send[v, step, n] = total.astype(BF16)
                sums_to(v, step, n, target, 2 * own_block, kpoints)

    def send_own(v):
        totals = screen(v, [sibling, me], whole)
        sending = sums_send.at[v, groups - 1, 0]
        sending[...] = totals[0].astype(BF16)
        slot = 2 * own_block + side
        remote(
            sending,
            sums_slot.at[v, slot],
            sums_send_sem.at[v],
            sums_recv_sem.at[v, kpoints],
            (sibling, band),
        ).start()
        sums_slot[v, slot] = totals[1].astype(BF16)


    def make_sigma(v):
        drain(sums_slot.at[v, pl.ds(0, 2 * count + 1)], sums_recv_sem.at[v, kpoints])
        for step in range(count):
            other = lax.rem(pair + step, count)
            for side_core in range(2):
                which = 2 * other + side_core
                total = sums_slot[v, 2 * which].astype(F32)
                if not step:
                    total += sums_slot[v, 2 * which + 1].astype(F32)
                lines = aligned(which * block, block)
                direct = 2.0 * potential[lines, v : v + 1] * occ[lines, :].astype(F32)
                coupling[v, lines, :] = (direct - total).astype(BF16)
        total = jnp.dot(vir_turned[...], coupling[v], preferred_element_type=F32)
        sigma_own[...] = total
        sigma_send[v] = total.astype(BF16)
        for way, peer in enumerate(others):
            remote(
                sigma_send.at[v, pl.ds(pl.multiple_of(peer * columns, 16), columns)],
                sigma_recv.at[v, way],
                sigma_sem.at[vectors],
                sigma_sem.at[v],
                (me, peer),
            ).start()
        out[v] = gaps[...] * trial[v] + sigma_own[pl.ds(pl.multiple_of(band * columns, 16), columns)]

    take_halves(0)
    drain(occ_tile.at[pl.ds(0, groups), pl.ds(0, width - piece)], occ_pass_sem.at[1])
    make_pairs(0, (band, near_x, near_y))
    for step in range(groups - 2):
        take_corner(step)
        if step == groups - 3:
            for position in range(groups - 2, groups):
                take_corner(position)
        screen_far(0, step, early)
    drain(occ_tile.at[pl.ds(0, groups), pl.ds(0, piece)], occ_pass_sem.at[2])
    make_pairs(0, (corner,))
    for step in range(groups - 2):
        screen_far(0, step, late, True)
        send_far(0, step)

    def both_far(v, step):
        screen_far(v, step, whole)
        send_far(v, step)

    sum_density()
    for v in range(1, vectors):
        take_halves(v)
        make_pairs(v, (band, near_x, near_y, corner))
        for step in range(groups - 2):
            both_far(v, step)
    for step in range(groups - 2):
        gather_far(0, step)
    both_far(0, groups - 2)
    gather_far(0, groups - 2)
    for v in range(1, vectors):
        both_far(v, groups - 2)
        for step in range(groups - 2):
            gather_far(v, step)
    for v in range(vectors):
        send_own(v)
        if v == 0:
            for later in range(1, vectors):
                gather_far(later, groups - 2)
            make_potential()
        make_sigma(v)
    for v in range(vectors):
        drain(sigma_recv.at[v], sigma_sem.at[v])
        result = out[v]
        for way in range(bands - 1):
            result += sigma_recv[v, way].astype(F32)
        out[v] = result

    drain(sigma_recv, trial_sem.at[vectors])
    drain(sigma_recv, sigma_sem.at[vectors])
    for copy in point_copies:
        copy.wait_send()
    drain(occ_tile.at[pl.ds(0, groups), pl.ds(0, width - piece)], occ_send_sem.at[0])
    drain(occ_tile.at[pl.ds(0, groups)], occ_pass_sem.at[0])
    drain(half_all.at[pl.ds(0, groups + 1)], half_send_sem.at[0])
    drain(dens_all.at[pl.ds(0, kpoints - 1)], dens_sem.at[0])
    drain(dens_band.at[pl.ds(0, bands - 1)], dens_band_sem.at[0])
    for v in range(vectors):
        drain(sums_slot.at[v, pl.ds(0, 2 * groups - 1)], sums_send_sem.at[v])
        for far in range(groups - 2):
            for owner_core in range(2):
                pl.when(passing(v, far_groups[far]))(half_pass(v, far, owner_core).wait_send)
    for copy, direct in direct_copies():
        pl.when(direct)(copy.wait_send)


def coupled_part(
    kpoints, bands, occ, vir, trial, occ_energy, vir_energy, coulomb, exch, table
):
    rows, occupied = occ.shape
    vectors, columns = trial.shape[:2]
    groups = kpoints // 2
    count = groups // 2
    block = rows // groups
    width = bands * rows // 2
    vmem = pl.BlockSpec(memory_space=pltpu.VMEM)
    hbm = pl.BlockSpec(memory_space=pltpu.HBM)
    dma = pltpu.SemaphoreType.DMA
    return pl.pallas_call(
        functools.partial(kernel, kpoints, bands, vectors),
        out_shape=pltpu.VMEM(trial.shape, F32),
        in_specs=[hbm] * 8,
        out_specs=vmem,
        scratch_shapes=[
            pltpu.VMEM(occ.shape, BF16),
            pltpu.VMEM(vir.shape, BF16),
            pltpu.VMEM(trial.shape, F32),
            pltpu.VMEM(occ_energy.shape, F32),
            pltpu.VMEM(vir_energy.shape, F32),
            pltpu.SMEM(table.shape, jnp.int32),
            pltpu.VMEM((columns, occupied), F32),
            pltpu.VMEM((kpoints, block, width), F32),
            pltpu.VMEM((vectors, bands * columns, occupied), BF16),
            pltpu.VMEM((bands * columns, rows), BF16),
            pltpu.VMEM((vectors, rows, occupied), BF16),
            pltpu.VMEM((kpoints, vectors * block, occupied), BF16),
            pltpu.VMEM((kpoints, width, occupied), BF16),
            pltpu.VMEM((kpoints, vectors, rows), F32),
            pltpu.VMEM((bands, vectors, rows), F32),
            pltpu.VMEM((rows, 128), F32),
            pltpu.VMEM(coulomb.shape, BF16),
            pltpu.VMEM((kpoints, block, width), BF16),
            pltpu.VMEM((kpoints, vectors * block, width), F32),
            pltpu.VMEM((vectors, groups - 1, 2, block, occupied), F32),
            pltpu.VMEM((vectors, groups, 2, block, occupied), BF16),
            pltpu.VMEM((vectors, 2 * groups + kpoints, block, occupied), BF16),
            pltpu.VMEM((vectors, rows, occupied), BF16),
            pltpu.VMEM((bands * columns, occupied), F32),
            pltpu.VMEM((vectors, bands * columns, occupied), BF16),
            pltpu.VMEM((vectors, bands - 1, columns, occupied), BF16),
            dma((8,)),
            dma((vectors + 1,)),
            dma((2, groups)),
            dma((1,)),
            dma((groups, bands - 1)),
            dma((3,)),
            dma((1,)),
            dma((vectors, kpoints)),
            dma((vectors, groups - 2, 2)),
            dma((count - 1, 2)),
            dma((2,)),
            dma((2,)),
            dma((vectors,)),
            dma((vectors, kpoints + 1)),
            dma((vectors + 1,)),
        ],
        compiler_params=pltpu.CompilerParams(
            collective_id=0, has_side_effects=True, vmem_limit_bytes=40 * 2**20
        ),
        name="coupled",
    )(
        *(
            pltpu.with_memory_space_constraint(given, pltpu.HBM)
            for given in (occ, vir, trial, occ_energy, vir_energy, coulomb, exch, table)
        )
    )


def per_device(
    occ_rows, vir_rows, trial_vectors, occ_energy, vir_energy, coulomb, exch_kernel, minus_table
):
    kpoints = lax.axis_size("ka")
    bands = lax.axis_size("band")
    trial_turned = jnp.swapaxes(trial_vectors[0], 1, 2)
    coupled = coupled_part(
        kpoints,
        bands,
        occ_rows[0],
        vir_rows[0],
        trial_turned,
        occ_energy,
        vir_energy,
        coulomb,
        exch_kernel,
        minus_table,
    )
    return jnp.swapaxes(coupled, 1, 2)[None]


def solution(mesh):
    in_specs = (
        P("ka", "band", None),
        P("ka", "band", None),
        P("ka", None, None, "band"),
        P("ka", None),
        P("ka", "band"),
        P("band", None),
        P(None, "band", None),
        P(),
    )
    out_specs = P("ka", None, None, "band")
    return jax.shard_map(
        per_device, mesh=mesh, in_specs=in_specs, out_specs=out_specs, check_vma=False
    )
```

```python
import functools

import jax
import jax.numpy as jnp
from jax import lax
from jax.experimental import pallas as pl
from jax.experimental.pallas import tpu as pltpu
from jax.sharding import PartitionSpec as P

F32 = jnp.float32
BF16 = jnp.bfloat16
CHUNK = 16
SPAN = 512


def dot_nt(left, right, **options):
    return lax.dot_general(
        left, right, (((1,), (1,)), ((), ())), preferred_element_type=F32, **options
    )


def aligned(start, size):
    return pl.ds(pl.multiple_of(start, size), size)


def kernel(
    kpoints,
    bands,
    vectors,
    occ_given,
    vir_given,
    trial_given,
    occ_energy_given,
    vir_energy_given,
    coulomb,
    exch,
    table_given,
    out,
    occ,
    vir,
    trial,
    occ_energy,
    vir_energy,
    table,
    gaps,
    exch_wide,
    trial_full,
    vir_turned,
    half_own,
    half_all,
    occ_tile,
    dens_all,
    dens_band,
    potential,
    coulomb_here,
    exch_tile,
    pairs,
    held,
    sums_send,
    sums_slot,
    coupling,
    sigma_own,
    sigma_send,
    sigma_recv,
    local_sem,
    trial_sem,
    point_sem,
    occ_send_sem,
    occ_sem,
    occ_pass_sem,
    half_send_sem,
    half_recv_sem,
    half_pass_sem,
    half_direct_sem,
    dens_sem,
    dens_band_sem,
    sums_send_sem,
    sums_recv_sem,
    sigma_sem,
):
    me = lax.axis_index("ka")
    band = lax.axis_index("band")
    groups = kpoints // 2
    count = groups // 2
    group = lax.div(me, 2)
    core = lax.rem(me, 2)
    sibling = me + 1 - 2 * core
    pair = lax.div(group, 2)
    side = lax.rem(group, 2)
    partner = group + 1 - 2 * side
    rows, occupied = occ.shape
    columns = trial.shape[1]
    block = rows // groups
    piece = rows // 2
    width = bands * piece
    near_x = band + 1 - 2 * lax.rem(band, 2)
    near_y = lax.rem(band + 2, bands)
    corner = bands - 1 - band
    others = (corner, near_x, near_y)

    def tile_of(k):
        return lax.rem(k, 2) * groups + lax.div(k, 2)

    def rank(k, home):
        return lax.select(k < 4 * home, k, k - 4)

    def remote(source, target, send, recv, device):
        return pltpu.make_async_remote_copy(
            src_ref=source,
            dst_ref=target,
            send_sem=send,
            recv_sem=recv,
            device_id=device,
            device_id_type=pl.DeviceIdType.MESH,
        )

    def arrival(target, recv):
        return remote(target, target, recv, recv, (sibling, band))

    def drain(held, sem):
        pltpu.make_async_copy(held, held, sem).wait()

    barrier = pltpu.get_barrier_semaphore()
    for peer in others:
        pl.semaphore_signal(
            barrier, inc=1, device_id=(me, peer), device_id_type=pl.DeviceIdType.MESH
        )
    for step in range(1, kpoints):
        pl.semaphore_signal(
            barrier,
            inc=1,
            device_id=(lax.rem(me + step, kpoints), band),
            device_id_type=pl.DeviceIdType.MESH,
        )

    load_copies = []
    for given, here in (
        (trial_given, trial),
        (occ_given, occ),
        (vir_given, vir),
        (table_given, table),
        (occ_energy_given, occ_energy),
        (vir_energy_given, vir_energy),
    ):
        copy = pltpu.make_async_copy(given, here, local_sem.at[2 + len(load_copies)])
        copy.start()
        load_copies.append(copy)
    trial_load, occ_load, vir_load, *other_loads = load_copies
    for part in range(bands):
        pltpu.make_async_copy(
            exch.at[
                :,
                aligned((2 * pair + core) * block, block),
                aligned(part * rows + side * piece, piece),
            ],
            exch_tile.at[:, :, pl.ds(part * piece, piece)],
            local_sem.at[1],
        ).start()
    coulomb_copy = pltpu.make_async_copy(coulomb, coulomb_here, local_sem.at[0])
    coulomb_copy.start()

    own_columns = aligned(band * columns, columns)
    trial_load.wait()
    trial_full[:, own_columns, :] = trial[...].astype(BF16)
    pl.semaphore_wait(barrier, len(others) + kpoints - 1)

    for v in range(vectors):
        for peer in others:
            remote(
                trial_full.at[v, own_columns],
                trial_full.at[v, own_columns],
                trial_sem.at[vectors],
                trial_sem.at[v],
                (me, peer),
            ).start()

    def piece_of(owner):
        return aligned(owner * piece, piece)

    far_groups = []
    for step in range(groups - 2):
        low = lax.rem(2 * pair + 2 + step, groups)
        high = lax.rem(2 * pair + 2 * groups - 1 - step, groups)
        far_groups.append(lax.select(2 * pair < count, low, high))
    far_groups.reverse()
    order = [group, partner] + far_groups

    mine = tile_of(me)
    occ_load.wait()
    for peer in order[1:]:
        copy = remote(
            occ.at[aligned(lax.rem(peer, 2) * piece, piece)],
            occ_tile.at[mine, piece_of(band)],
            point_sem.at[groups],
            point_sem.at[group],
            (peer * 2 + core, band),
        )
        copy.start()
    occ_tile[mine, piece_of(band), :] = occ[aligned(side * piece, piece), :]

    def occ_out(source_group):
        tile = core * groups + source_group
        here = occ_tile.at[tile, piece_of(band)]
        for way, peer in ((1, near_x), (2, near_y)):
            remote(
                here,
                here,
                occ_send_sem.at[0],
                occ_sem.at[source_group, 0],
                (me, peer),
            ).start()
        occ_pass(source_group, 0, band).start()

    def occ_pass(source_group, way, owner):
        here = occ_tile.at[core * groups + source_group, piece_of(owner)]
        return remote(
            here,
            here,
            occ_pass_sem.at[0],
            occ_pass_sem.at[1 + way // (bands - 1)],
            (sibling, band),
        )

    occ_out(group)
    vir_load.wait()
    vir_turned[...] = vir[...].T
    for copy in other_loads:
        copy.wait()
    turned = jnp.broadcast_to(vir_energy[...], (occupied, columns)).T
    gaps[...] = turned - occ_energy[...]
    drain(exch_tile, local_sem.at[1])

    def widen(k, carry):
        exch_wide[k] = exch_tile[k].astype(F32)
        return carry

    lax.fori_loop(0, kpoints, widen, 0)

    def take_point(source_group):
        arrival(
            occ_tile.at[core * groups + source_group, piece_of(band)],
            point_sem.at[source_group],
        ).wait_recv()
        occ_out(source_group)

    def own_half(v):
        drain(sigma_recv.at[v], trial_sem.at[v])
        half_own[v] = jnp.dot(vir[...], trial_full[v], preferred_element_type=F32).astype(BF16)
        lines = pl.ds(v * block, block)
        own_block = 2 * pair + core
        half_all[me, lines, :] = half_own[v, aligned(own_block * block, block), :]
        destinations = []
        for step in range(1, count):
            other = lax.rem(pair + step, count)
            near = lax.select(other > pair, 2 * other, 2 * other + 1)
            destinations += [
                (2 * other + side_core, near * 2 + side_core, rank(me, other))
                for side_core in range(2)
            ]
        destinations += [
            (2 * pair + side_core, partner * 2 + side_core, kpoints - 4) for side_core in range(2)
        ]
        destinations.append((2 * pair + 1 - core, sibling, kpoints - 4))
        for which, device, slot in destinations:
            remote(
                half_own.at[v, aligned(which * block, block)],
                half_all.at[me, lines],
                half_send_sem.at[0],
                half_recv_sem.at[v, slot],
                (device, band),
            ).start()
        if v == 0:
            for copy, direct in direct_copies():
                pl.when(direct)(copy.start)

    def direct_copies():
        copies = []
        for step in range(1, count):
            other = lax.rem(pair + step, count)
            above = other > pair
            distant = lax.select(above, 2 * other + 1, 2 * other)
            for side_core in range(2):
                copy = remote(
                    half_own.at[0, aligned((2 * other + side_core) * block, block)],
                    half_all.at[me, pl.ds(0, block)],
                    half_direct_sem.at[step - 1, side_core],
                    half_recv_sem.at[0, rank(me, other)],
                    (distant * 2 + side_core, band),
                )
                copies.append((copy, lax.select(above, side, 1 - side) == 1))
        return copies

    def half_pass(v, position, owner_core):
        source = far_groups[position] * 2 + owner_core
        here = half_all.at[source, pl.ds(v * block, block)]
        return remote(
            here,
            here,
            half_pass_sem.at[v, position, owner_core],
            half_recv_sem.at[v, rank(source, pair)],
            (partner * 2 + core, band),
        )

    def take_half(v, source):
        here = half_all.at[source, pl.ds(v * block, block)]
        arrival(here, half_recv_sem.at[v, rank(source, pair)]).wait_recv()

    def passing(v, source_group):
        below = source_group < 2 * pair
        near = lax.select(below, 1 - side, side)
        if v:
            return near == 1
        source_side = lax.rem(source_group, 2)
        return near * lax.select(below, 1 - source_side, source_side) == 1

    def take_far(v, position):
        for owner_core in range(2):
            take_half(v, far_groups[position] * 2 + owner_core)
            pl.when(passing(v, far_groups[position]))(half_pass(v, position, owner_core).start)

    def occ_turn(position):
        source_group = order[position]
        tile = core * groups + source_group
        if position < groups // 2:
            owner, onward = near_x, near_y
        else:
            owner, onward = near_y, near_x
        here = occ_tile.at[tile, piece_of(owner)]
        return remote(
            here,
            here,
            occ_send_sem.at[0],
            occ_sem.at[source_group, 1],
            (me, onward),
        )

    def occ_in(position):
        source_group = order[position]
        tile = core * groups + source_group
        drain(occ_tile.at[tile, pl.ds(0, 2 * piece)], occ_sem.at[source_group, 0])
        occ_turn(position).start()
        for way, owner in ((1, near_x), (2, near_y)):
            occ_pass(source_group, way, owner).start()

    inner = lax.select(2 * pair < count, side, 1 - side) == 1

    take_point(partner)
    for v in range(vectors):
        own_half(v)
        for source_group in far_groups[v::vectors]:
            take_point(source_group)
    for position in range(groups):
        occ_in(position)
        if position < groups - 2:

            @pl.when(inner)
            def _(far=position):
                take_far(0, far)

    ones = jnp.ones((8, occupied), F32)
    occ_wide = occ[...].astype(F32)
    dens_all[me] = jnp.concatenate(
        [
            dot_nt(ones, occ_wide * half_own[v].astype(F32), precision=lax.Precision.HIGHEST)[:1]
            for v in range(vectors)
        ],
        axis=0,
    )
    for step in range(1, kpoints):
        remote(
            dens_all.at[me],
            dens_all.at[me],
            dens_sem.at[0],
            dens_sem.at[1],
            (lax.rem(me + step, kpoints), band),
        ).start()

    @pl.when(inner)
    def _():
        for v in range(1, vectors):
            for far in range(groups - 2):
                take_far(v, far)

    def take_corner(position):
        source_group = order[position]
        here = occ_tile.at[core * groups + source_group, piece_of(corner)]
        arrival(here, occ_sem.at[source_group, 1]).wait_recv()
        occ_pass(source_group, bands - 1, corner).start()

    def take_halves(v):
        drain(half_all.at[pl.ds(0, 3), pl.ds(v * block, block)], half_recv_sem.at[v, kpoints - 4])

        @pl.when(jnp.logical_not(inner))
        def _():
            for far in range(groups - 2):
                take_far(v, far)

    def make_pairs(v, owners):
        lines = pl.ds(v * block, block)
        for source in range(kpoints):
            tile = tile_of(source)
            if len(owners) == bands:
                pairs[source, lines] = dot_nt(half_all[source, lines], occ_tile[tile])
                continue
            for owner in owners:
                part = piece_of(owner)
                pairs[source, lines, part] = dot_nt(
                    half_all[source, lines], occ_tile[tile, part]
                )

    def sum_density():
        drain(dens_all.at[pl.ds(0, kpoints - 1)], dens_sem.at[1])
        density = dens_all[0]
        for k in range(1, kpoints):
            density += dens_all[k]
        dens_band[band] = density
        for peer in others:
            remote(
                dens_band.at[band],
                dens_band.at[band],
                dens_band_sem.at[0],
                dens_band_sem.at[1],
                (me, peer),
            ).start()

    def make_potential():
        drain(dens_band.at[pl.ds(0, bands - 1)], dens_band_sem.at[1])
        coulomb_copy.wait()
        spread = jnp.zeros((16 - vectors, rows), F32)
        total = jnp.zeros((rows, 16), F32)
        for part in range(bands):
            here = jnp.concatenate([dens_band[part], spread], axis=0).astype(BF16)
            total += dot_nt(coulomb_here[:, part * rows : (part + 1) * rows], here)
        potential[:, :16] = total

    def screen(v, targets, spans):
        sources = [[table[target, q] for q in range(kpoints)] for target in targets]
        results = [jnp.zeros((block, occupied), F32) for _ in targets]
        for across, span in spans:
            chunks = [[] for _ in targets]
            for start in range(0, block, CHUNK):
                totals = [jnp.zeros((CHUNK, span), F32) for _ in targets]
                for q in range(kpoints):
                    factor = exch_wide[q, pl.ds(start, CHUNK), across]
                    for n in range(len(targets)):
                        there = pl.ds(v * block + start, CHUNK)
                        totals[n] += pairs[sources[n][q], there, across] * factor
                for n in range(len(targets)):
                    chunks[n].append(totals[n].astype(BF16))
            for n, target in enumerate(targets):
                results[n] += jnp.dot(
                    jnp.concatenate(chunks[n], axis=0),
                    occ_tile[tile_of(target), across],
                    preferred_element_type=F32,
                )
        return results

    whole = [(pl.ds(first, SPAN), SPAN) for first in range(0, width, SPAN)]
    early = [(piece_of(owner), piece) for owner in (band, near_x, near_y)]
    late = [(piece_of(corner), piece)]

    own_block = 2 * pair + core
    lower = 2 * pair
    higher = groups - 2 - lower
    outward = lax.select(side == 0, higher, lower)

    def far_target(step):
        rising = lax.select(step <= higher, groups - 1 - step, step - higher - 1)
        falling = lax.select(step <= lower, step, groups + lower - step)
        return lax.select(side == 0, rising, falling)

    def sums_to(v, step, n, device, slot, recv):
        remote(
            sums_send.at[v, step, n],
            sums_slot.at[v, slot],
            sums_send_sem.at[v],
            sums_recv_sem.at[v, recv],
            (device, band),
        ).start()

    def screen_far(v, step, spans, before=None):
        target_group = far_target(step)
        totals = screen(v, [target_group * 2 + n for n in range(2)], spans)
        for n in range(2):
            held[v, step, n] = totals[n] if before is None else held[v, step, n] + totals[n]

    def send_far(v, step):
        target_group = far_target(step)
        through = step < outward

        @pl.when(step <= outward)
        def _():
            for n in range(2):
                target = target_group * 2 + n
                sums_send[v, step, n] = held[v, step, n].astype(BF16)
                sums_to(
                    v,
                    step,
                    n,
                    lax.select(through, partner * 2 + core, target),
                    lax.select(through, 2 * groups + target, 2 * own_block + side),
                    lax.select(through, rank(target, pair), kpoints - 4),
                )

    def gather_far(v, step):
        @pl.when(step > outward)
        def _():
            for n in range(2):
                target = far_target(step) * 2 + n
                before = sums_slot.at[v, 2 * groups + target]
                arrival(before, sums_recv_sem.at[v, rank(target, pair)]).wait_recv()
                total = held[v, step, n] + before[...].astype(F32)
                sums_send[v, step, n] = total.astype(BF16)
                sums_to(v, step, n, target, 2 * own_block, kpoints - 4)

    def send_own(v):
        totals = screen(v, [sibling, me], whole)
        sending = sums_send.at[v, groups - 1, 0]
        sending[...] = totals[0].astype(BF16)
        slot = 2 * own_block + side
        remote(
            sending,
            sums_slot.at[v, slot],
            sums_send_sem.at[v],
            sums_recv_sem.at[v, kpoints - 4],
            (sibling, band),
        ).start()
        sums_slot[v, slot] = totals[1].astype(BF16)


    def make_sigma(v):
        drain(sums_slot.at[v, pl.ds(0, 2 * count + 1)], sums_recv_sem.at[v, kpoints - 4])
        for step in range(count):
            other = lax.rem(pair + step, count)
            for side_core in range(2):
                which = 2 * other + side_core
                total = sums_slot[v, 2 * which].astype(F32)
                if not step:
                    total += sums_slot[v, 2 * which + 1].astype(F32)
                lines = aligned(which * block, block)
                direct = 2.0 * potential[lines, v : v + 1] * occ[lines, :].astype(F32)
                coupling[v, lines, :] = (direct - total).astype(BF16)
        total = jnp.dot(vir_turned[...], coupling[v], preferred_element_type=F32)
        sigma_own[...] = total
        sigma_send[v] = total.astype(BF16)
        for way, peer in enumerate(others):
            remote(
                sigma_send.at[v, pl.ds(pl.multiple_of(peer * columns, 16), columns)],
                sigma_recv.at[v, way],
                sigma_sem.at[vectors],
                sigma_sem.at[v],
                (me, peer),
            ).start()
        out[v] = gaps[...] * trial[v] + sigma_own[pl.ds(pl.multiple_of(band * columns, 16), columns)]

    take_halves(0)
    drain(occ_tile.at[pl.ds(0, groups), pl.ds(0, width - piece)], occ_pass_sem.at[1])
    make_pairs(0, (band, near_x, near_y))
    for step in range(groups - 2):
        take_corner(step)
        if step == groups - 3:
            for position in range(groups - 2, groups):
                take_corner(position)
        screen_far(0, step, early)
    drain(occ_tile.at[pl.ds(0, groups), pl.ds(0, piece)], occ_pass_sem.at[2])
    make_pairs(0, (corner,))
    for step in range(groups - 2):
        screen_far(0, step, late, True)
        send_far(0, step)

    def both_far(v, step):
        screen_far(v, step, whole)
        send_far(v, step)

    sum_density()
    for v in range(1, vectors):
        take_halves(v)
        make_pairs(v, (band, near_x, near_y, corner))
        for step in range(groups - 2):
            both_far(v, step)
    for step in range(groups - 2):
        gather_far(0, step)
    both_far(0, groups - 2)
    gather_far(0, groups - 2)
    for v in range(1, vectors):
        both_far(v, groups - 2)
        for step in range(groups - 2):
            gather_far(v, step)
    for v in range(vectors):
        send_own(v)
        if v == 0:
            for later in range(1, vectors):
                gather_far(later, groups - 2)
            make_potential()
        make_sigma(v)
    for v in range(vectors):
        drain(sigma_recv.at[v], sigma_sem.at[v])
        result = out[v]
        for way in range(bands - 1):
            result += sigma_recv[v, way].astype(F32)
        out[v] = result

    drain(sigma_recv, trial_sem.at[vectors])
    drain(sigma_recv, sigma_sem.at[vectors])
    drain(
        exch_tile.at[pl.ds(0, groups - 1), pl.ds(0, occupied // bands)], point_sem.at[groups]
    )
    drain(occ_tile.at[pl.ds(0, groups), pl.ds(0, width - piece)], occ_send_sem.at[0])
    drain(occ_tile.at[pl.ds(0, groups)], occ_pass_sem.at[0])
    drain(half_all.at[pl.ds(0, groups + 1)], half_send_sem.at[0])
    drain(dens_all.at[pl.ds(0, kpoints - 1)], dens_sem.at[0])
    drain(dens_band.at[pl.ds(0, bands - 1)], dens_band_sem.at[0])
    for v in range(vectors):
        drain(sums_slot.at[v, pl.ds(0, 2 * groups - 1)], sums_send_sem.at[v])
        for far in range(groups - 2):
            for owner_core in range(2):
                pl.when(passing(v, far_groups[far]))(half_pass(v, far, owner_core).wait_send)
    for copy, direct in direct_copies():
        pl.when(direct)(copy.wait_send)


def coupled_part(
    kpoints, bands, occ, vir, trial, occ_energy, vir_energy, coulomb, exch, table
):
    rows, occupied = occ.shape
    vectors, columns = trial.shape[:2]
    groups = kpoints // 2
    count = groups // 2
    block = rows // groups
    width = bands * rows // 2
    vmem = pl.BlockSpec(memory_space=pltpu.VMEM)
    hbm = pl.BlockSpec(memory_space=pltpu.HBM)
    dma = pltpu.SemaphoreType.DMA
    return pl.pallas_call(
        functools.partial(kernel, kpoints, bands, vectors),
        out_shape=pltpu.VMEM(trial.shape, F32),
        in_specs=[hbm] * 8,
        out_specs=vmem,
        scratch_shapes=[
            pltpu.VMEM(occ.shape, BF16),
            pltpu.VMEM(vir.shape, BF16),
            pltpu.VMEM(trial.shape, F32),
            pltpu.VMEM(occ_energy.shape, F32),
            pltpu.VMEM(vir_energy.shape, F32),
            pltpu.SMEM(table.shape, jnp.int32),
            pltpu.VMEM((columns, occupied), F32),
            pltpu.VMEM((kpoints, block, width), F32),
            pltpu.VMEM((vectors, bands * columns, occupied), BF16),
            pltpu.VMEM((bands * columns, rows), BF16),
            pltpu.VMEM((vectors, rows, occupied), BF16),
            pltpu.VMEM((kpoints, vectors * block, occupied), BF16),
            pltpu.VMEM((kpoints, width, occupied), BF16),
            pltpu.VMEM((kpoints, vectors, rows), F32),
            pltpu.VMEM((bands, vectors, rows), F32),
            pltpu.VMEM((rows, 128), F32),
            pltpu.VMEM(coulomb.shape, BF16),
            pltpu.VMEM((kpoints, block, width), BF16),
            pltpu.VMEM((kpoints, vectors * block, width), F32),
            pltpu.VMEM((vectors, groups - 1, 2, block, occupied), F32),
            pltpu.VMEM((vectors, groups, 2, block, occupied), BF16),
            pltpu.VMEM((vectors, 2 * groups + kpoints, block, occupied), BF16),
            pltpu.VMEM((vectors, rows, occupied), BF16),
            pltpu.VMEM((bands * columns, occupied), F32),
            pltpu.VMEM((vectors, bands * columns, occupied), BF16),
            pltpu.VMEM((vectors, bands - 1, columns, occupied), BF16),
            dma((8,)),
            dma((vectors + 1,)),
            dma((groups + 1,)),
            dma((1,)),
            dma((groups, 2)),
            dma((3,)),
            dma((1,)),
            dma((vectors, kpoints - 3)),
            dma((vectors, groups - 2, 2)),
            dma((count - 1, 2)),
            dma((2,)),
            dma((2,)),
            dma((vectors,)),
            dma((vectors, kpoints - 3)),
            dma((vectors + 1,)),
        ],
        compiler_params=pltpu.CompilerParams(
            collective_id=0, has_side_effects=True, vmem_limit_bytes=40 * 2**20
        ),
        name="coupled",
    )(
        *(
            pltpu.with_memory_space_constraint(given, pltpu.HBM)
            for given in (occ, vir, trial, occ_energy, vir_energy, coulomb, exch, table)
        )
    )


def per_device(
    occ_rows, vir_rows, trial_vectors, occ_energy, vir_energy, coulomb, exch_kernel, minus_table
):
    kpoints = lax.axis_size("ka")
    bands = lax.axis_size("band")
    trial_turned = jnp.swapaxes(trial_vectors[0], 1, 2)
    coupled = coupled_part(
        kpoints,
        bands,
        occ_rows[0],
        vir_rows[0],
        trial_turned,
        occ_energy,
        vir_energy,
        coulomb,
        exch_kernel,
        minus_table,
    )
    return jnp.swapaxes(coupled, 1, 2)[None]


def solution(mesh):
    in_specs = (
        P("ka", "band", None),
        P("ka", "band", None),
        P("ka", None, None, "band"),
        P("ka", None),
        P("ka", "band"),
        P("band", None),
        P(None, "band", None),
        P(),
    )
    out_specs = P("ka", None, None, "band")
    return jax.shard_map(
        per_device, mesh=mesh, in_specs=in_specs, out_specs=out_specs, check_vma=False
    )
```

```python
import functools

import jax
import jax.numpy as jnp
from jax import lax
from jax.experimental import pallas as pl
from jax.experimental.pallas import tpu as pltpu
from jax.sharding import PartitionSpec as P

F32 = jnp.float32
BF16 = jnp.bfloat16
CHUNK = 16
SPAN = 512


def dot_nt(left, right, **options):
    return lax.dot_general(
        left, right, (((1,), (1,)), ((), ())), preferred_element_type=F32, **options
    )


def aligned(start, size):
    return pl.ds(pl.multiple_of(start, size), size)


def kernel(
    kpoints,
    bands,
    vectors,
    occ_given,
    vir_given,
    trial_given,
    occ_energy_given,
    vir_energy_given,
    coulomb,
    exch,
    table_given,
    out,
    occ,
    vir,
    trial,
    occ_energy,
    vir_energy,
    table,
    gaps,
    exch_wide,
    trial_full,
    vir_turned,
    half_own,
    half_all,
    occ_tile,
    dens_all,
    dens_band,
    potential,
    coulomb_here,
    exch_tile,
    pairs,
    held,
    sums_send,
    sums_slot,
    coupling,
    sigma_own,
    sigma_send,
    sigma_recv,
    local_sem,
    trial_sem,
    point_sem,
    occ_send_sem,
    occ_sem,
    occ_pass_sem,
    half_send_sem,
    half_recv_sem,
    half_pass_sem,
    half_direct_sem,
    dens_sem,
    dens_band_sem,
    sums_send_sem,
    sums_recv_sem,
    sigma_sem,
):
    me = lax.axis_index("ka")
    band = lax.axis_index("band")
    groups = kpoints // 2
    count = groups // 2
    group = lax.div(me, 2)
    core = lax.rem(me, 2)
    sibling = me + 1 - 2 * core
    pair = lax.div(group, 2)
    side = lax.rem(group, 2)
    partner = group + 1 - 2 * side
    rows, occupied = occ.shape
    columns = trial.shape[1]
    block = rows // groups
    piece = rows // 2
    width = bands * piece
    near_x = band + 1 - 2 * lax.rem(band, 2)
    near_y = lax.rem(band + 2, bands)
    corner = bands - 1 - band
    others = (corner, near_x, near_y)

    def tile_of(k):
        return lax.rem(k, 2) * groups + lax.div(k, 2)

    def rank(k, home):
        return lax.select(k < 4 * home, k, k - 4)

    def remote(source, target, send, recv, device):
        return pltpu.make_async_remote_copy(
            src_ref=source,
            dst_ref=target,
            send_sem=send,
            recv_sem=recv,
            device_id=device,
            device_id_type=pl.DeviceIdType.MESH,
        )

    def arrival(target, recv):
        return remote(target, target, recv, recv, (sibling, band))

    def piece_at(way):
        return pl.ds(way * piece, piece)

    def drain(held, sem):
        pltpu.make_async_copy(held, held, sem).wait()

    barrier = pltpu.get_barrier_semaphore()
    for peer in others:
        pl.semaphore_signal(
            barrier, inc=1, device_id=(me, peer), device_id_type=pl.DeviceIdType.MESH
        )
    for step in range(1, kpoints):
        pl.semaphore_signal(
            barrier,
            inc=1,
            device_id=(lax.rem(me + step, kpoints), band),
            device_id_type=pl.DeviceIdType.MESH,
        )

    load_copies = []
    for given, here in (
        (trial_given, trial),
        (occ_given, occ),
        (vir_given, vir),
        (table_given, table),
        (occ_energy_given, occ_energy),
        (vir_energy_given, vir_energy),
    ):
        copy = pltpu.make_async_copy(given, here, local_sem.at[2 + len(load_copies)])
        copy.start()
        load_copies.append(copy)
    trial_load, occ_load, vir_load, *other_loads = load_copies
    for way, owner in enumerate((band, near_x, near_y, corner)):
        pltpu.make_async_copy(
            exch.at[
                :,
                aligned((2 * pair + core) * block, block),
                aligned(owner * rows + side * piece, piece),
            ],
            exch_tile.at[:, :, piece_at(way)],
            local_sem.at[1],
        ).start()
    coulomb_copy = pltpu.make_async_copy(coulomb, coulomb_here, local_sem.at[0])
    coulomb_copy.start()

    own_columns = aligned(band * columns, columns)
    trial_load.wait()
    trial_full[:, own_columns, :] = trial[...].astype(BF16)
    pl.semaphore_wait(barrier, len(others) + kpoints - 1)

    for v in range(vectors):
        for peer in others:
            remote(
                trial_full.at[v, own_columns],
                trial_full.at[v, own_columns],
                trial_sem.at[vectors],
                trial_sem.at[v],
                (me, peer),
            ).start()

    far_groups = []
    for step in range(groups - 2):
        low = lax.rem(2 * pair + 2 + step, groups)
        high = lax.rem(2 * pair + 2 * groups - 1 - step, groups)
        far_groups.append(lax.select(2 * pair < count, low, high))
    far_groups.reverse()
    order = [group, partner] + far_groups

    mine = tile_of(me)
    occ_load.wait()
    for peer in order[1:]:
        copy = remote(
            occ.at[aligned(lax.rem(peer, 2) * piece, piece)],
            occ_tile.at[mine, piece_at(0)],
            point_sem.at[groups],
            point_sem.at[group],
            (peer * 2 + core, band),
        )
        copy.start()
    occ_tile[mine, piece_at(0), :] = occ[aligned(side * piece, piece), :]

    def occ_out(source_group):
        tile = core * groups + source_group
        here = occ_tile.at[tile, piece_at(0)]
        for way, peer in ((1, near_x), (2, near_y)):
            remote(
                here,
                occ_tile.at[tile, piece_at(way)],
                occ_send_sem.at[0],
                occ_sem.at[source_group, 0],
                (me, peer),
            ).start()
        occ_pass(source_group, 0).start()

    def occ_pass(source_group, way, pieces=1):
        here = occ_tile.at[core * groups + source_group, pl.ds(way * piece, pieces * piece)]
        return remote(
            here,
            here,
            occ_pass_sem.at[0],
            occ_pass_sem.at[1 + way // (bands - 1)],
            (sibling, band),
        )

    occ_out(group)
    vir_load.wait()
    vir_turned[...] = vir[...].T
    for copy in other_loads:
        copy.wait()
    turned = jnp.broadcast_to(vir_energy[...], (occupied, columns)).T
    gaps[...] = turned - occ_energy[...]
    drain(exch_tile, local_sem.at[1])

    def widen(k, carry):
        exch_wide[k] = exch_tile[k].astype(F32)
        return carry

    lax.fori_loop(0, kpoints, widen, 0)

    def take_point(source_group):
        arrival(
            occ_tile.at[core * groups + source_group, piece_at(0)],
            point_sem.at[source_group],
        ).wait_recv()
        occ_out(source_group)

    def own_half(v):
        drain(sigma_recv.at[v], trial_sem.at[v])
        half_own[v] = jnp.dot(vir[...], trial_full[v], preferred_element_type=F32).astype(BF16)
        lines = pl.ds(v * block, block)
        own_block = 2 * pair + core
        half_all[me, lines, :] = half_own[v, aligned(own_block * block, block), :]
        destinations = []
        for step in range(1, count):
            other = lax.rem(pair + step, count)
            near = lax.select(other > pair, 2 * other, 2 * other + 1)
            destinations += [
                (2 * other + side_core, near * 2 + side_core, rank(me, other))
                for side_core in range(2)
            ]
        destinations += [
            (2 * pair + side_core, partner * 2 + side_core, kpoints - 4) for side_core in range(2)
        ]
        destinations.append((2 * pair + 1 - core, sibling, kpoints - 4))
        for which, device, slot in destinations:
            remote(
                half_own.at[v, aligned(which * block, block)],
                half_all.at[me, lines],
                half_send_sem.at[0],
                half_recv_sem.at[v, slot],
                (device, band),
            ).start()
        if v == 0:
            for copy, direct in direct_copies():
                pl.when(direct)(copy.start)

    def direct_copies():
        copies = []
        for step in range(1, count):
            other = lax.rem(pair + step, count)
            above = other > pair
            distant = lax.select(above, 2 * other + 1, 2 * other)
            for side_core in range(2):
                copy = remote(
                    half_own.at[0, aligned((2 * other + side_core) * block, block)],
                    half_all.at[me, pl.ds(0, block)],
                    half_direct_sem.at[step - 1, side_core],
                    half_recv_sem.at[0, rank(me, other)],
                    (distant * 2 + side_core, band),
                )
                copies.append((copy, lax.select(above, side, 1 - side) == 1))
        return copies

    def half_pass(v, position, owner_core):
        source = far_groups[position] * 2 + owner_core
        here = half_all.at[source, pl.ds(v * block, block)]
        return remote(
            here,
            here,
            half_pass_sem.at[v, position, owner_core],
            half_recv_sem.at[v, rank(source, pair)],
            (partner * 2 + core, band),
        )

    def take_half(v, source):
        here = half_all.at[source, pl.ds(v * block, block)]
        arrival(here, half_recv_sem.at[v, rank(source, pair)]).wait_recv()

    def passing(v, source_group):
        below = source_group < 2 * pair
        near = lax.select(below, 1 - side, side)
        if v:
            return near == 1
        source_side = lax.rem(source_group, 2)
        return near * lax.select(below, 1 - source_side, source_side) == 1

    def take_far(v, position):
        for owner_core in range(2):
            take_half(v, far_groups[position] * 2 + owner_core)
            pl.when(passing(v, far_groups[position]))(half_pass(v, position, owner_core).start)

    def occ_turn(position):
        source_group = order[position]
        tile = core * groups + source_group
        way, onward = (1, near_y) if position < groups // 2 else (2, near_x)
        return remote(
            occ_tile.at[tile, piece_at(way)],
            occ_tile.at[tile, piece_at(bands - 1)],
            occ_send_sem.at[0],
            occ_sem.at[source_group, 1],
            (me, onward),
        )

    def occ_in(position):
        source_group = order[position]
        tile = core * groups + source_group
        drain(occ_tile.at[tile, pl.ds(0, 2 * piece)], occ_sem.at[source_group, 0])
        occ_turn(position).start()
        occ_pass(source_group, 1, 2).start()

    inner = lax.select(2 * pair < count, side, 1 - side) == 1

    take_point(partner)
    for v in range(vectors):
        own_half(v)
        for source_group in far_groups[v::vectors]:
            take_point(source_group)
    for position in range(groups):
        occ_in(position)
        if position < groups - 2:

            @pl.when(inner)
            def _(far=position):
                take_far(0, far)

    ones = jnp.ones((8, occupied), F32)
    occ_wide = occ[...].astype(F32)
    dens_all[me] = jnp.concatenate(
        [
            dot_nt(ones, occ_wide * half_own[v].astype(F32), precision=lax.Precision.HIGHEST)[:1]
            for v in range(vectors)
        ],
        axis=0,
    )
    for step in range(1, kpoints):
        remote(
            dens_all.at[me],
            dens_all.at[me],
            dens_sem.at[0],
            dens_sem.at[1],
            (lax.rem(me + step, kpoints), band),
        ).start()

    @pl.when(inner)
    def _():
        for v in range(1, vectors):
            for far in range(groups - 2):
                take_far(v, far)

    def take_corner(position):
        source_group = order[position]
        here = occ_tile.at[core * groups + source_group, piece_at(bands - 1)]
        arrival(here, occ_sem.at[source_group, 1]).wait_recv()
        occ_pass(source_group, bands - 1).start()

    def take_halves(v):
        drain(half_all.at[pl.ds(0, 3), pl.ds(v * block, block)], half_recv_sem.at[v, kpoints - 4])

        @pl.when(jnp.logical_not(inner))
        def _():
            for far in range(groups - 2):
                take_far(v, far)

    def make_pairs(v, first, size):
        lines, part = pl.ds(v * block, block), pl.ds(first, size)
        for source in range(kpoints):
            pairs[source, lines, part] = dot_nt(
                half_all[source, lines], occ_tile[tile_of(source), part]
            )

    def sum_density():
        drain(dens_all.at[pl.ds(0, kpoints - 1)], dens_sem.at[1])
        density = dens_all[0]
        for k in range(1, kpoints):
            density += dens_all[k]
        dens_band[band] = density
        for peer in others:
            remote(
                dens_band.at[band],
                dens_band.at[band],
                dens_band_sem.at[0],
                dens_band_sem.at[1],
                (me, peer),
            ).start()

    def make_potential():
        drain(dens_band.at[pl.ds(0, bands - 1)], dens_band_sem.at[1])
        coulomb_copy.wait()
        spread = jnp.zeros((16 - vectors, rows), F32)
        total = jnp.zeros((rows, 16), F32)
        for part in range(bands):
            here = jnp.concatenate([dens_band[part], spread], axis=0).astype(BF16)
            total += dot_nt(coulomb_here[:, part * rows : (part + 1) * rows], here)
        potential[:, :16] = total

    def screen(v, targets, parts):
        sources = [[table[target, q] for q in range(kpoints)] for target in targets]
        results = [jnp.zeros((block, occupied), F32) for _ in targets]
        for across, span in parts:
            chunks = [[] for _ in targets]
            for start in range(0, block, CHUNK):
                totals = [jnp.zeros((CHUNK, span), F32) for _ in targets]
                for q in range(kpoints):
                    factor = exch_wide[q, pl.ds(start, CHUNK), across]
                    for n in range(len(targets)):
                        there = pl.ds(v * block + start, CHUNK)
                        totals[n] += pairs[sources[n][q], there, across] * factor
                for n in range(len(targets)):
                    chunks[n].append(totals[n].astype(BF16))
            for n, target in enumerate(targets):
                results[n] += jnp.dot(
                    jnp.concatenate(chunks[n], axis=0),
                    occ_tile[tile_of(target), across],
                    preferred_element_type=F32,
                )
        return results

    def spans(first, last):
        starts = range(first, last, SPAN)
        return [(pl.ds(start, min(SPAN, last - start)), min(SPAN, last - start)) for start in starts]

    whole = spans(0, width)
    early = spans(0, width - piece)
    late = spans(width - piece, width)

    own_block = 2 * pair + core
    lower = 2 * pair
    higher = groups - 2 - lower
    outward = lax.select(side == 0, higher, lower)

    def far_target(step):
        rising = lax.select(step <= higher, groups - 1 - step, step - higher - 1)
        falling = lax.select(step <= lower, step, groups + lower - step)
        return lax.select(side == 0, rising, falling)

    def sums_to(v, step, n, device, slot, recv):
        remote(
            sums_send.at[v, step, n],
            sums_slot.at[v, slot],
            sums_send_sem.at[v],
            sums_recv_sem.at[v, recv],
            (device, band),
        ).start()

    def screen_far(v, step, parts, before=None):
        target_group = far_target(step)
        totals = screen(v, [target_group * 2 + n for n in range(2)], parts)
        for n in range(2):
            held[v, step, n] = totals[n] if before is None else held[v, step, n] + totals[n]

    def send_far(v, step):
        target_group = far_target(step)
        through = step < outward

        @pl.when(step <= outward)
        def _():
            for n in range(2):
                target = target_group * 2 + n
                sums_send[v, step, n] = held[v, step, n].astype(BF16)
                sums_to(
                    v,
                    step,
                    n,
                    lax.select(through, partner * 2 + core, target),
                    lax.select(through, 2 * groups + target, 2 * own_block + side),
                    lax.select(through, rank(target, pair), kpoints - 4),
                )

    def gather_far(v, step):
        @pl.when(step > outward)
        def _():
            for n in range(2):
                target = far_target(step) * 2 + n
                before = sums_slot.at[v, 2 * groups + target]
                arrival(before, sums_recv_sem.at[v, rank(target, pair)]).wait_recv()
                total = held[v, step, n] + before[...].astype(F32)
                sums_send[v, step, n] = total.astype(BF16)
                sums_to(v, step, n, target, 2 * own_block, kpoints - 4)

    def send_own(v):
        totals = screen(v, [sibling, me], whole)
        sending = sums_send.at[v, groups - 1, 0]
        sending[...] = totals[0].astype(BF16)
        slot = 2 * own_block + side
        remote(
            sending,
            sums_slot.at[v, slot],
            sums_send_sem.at[v],
            sums_recv_sem.at[v, kpoints - 4],
            (sibling, band),
        ).start()
        sums_slot[v, slot] = totals[1].astype(BF16)


    def make_sigma(v):
        drain(sums_slot.at[v, pl.ds(0, 2 * count + 1)], sums_recv_sem.at[v, kpoints - 4])
        for step in range(count):
            other = lax.rem(pair + step, count)
            for side_core in range(2):
                which = 2 * other + side_core
                total = sums_slot[v, 2 * which].astype(F32)
                if not step:
                    total += sums_slot[v, 2 * which + 1].astype(F32)
                lines = aligned(which * block, block)
                direct = 2.0 * potential[lines, v : v + 1] * occ[lines, :].astype(F32)
                coupling[v, lines, :] = (direct - total).astype(BF16)
        total = jnp.dot(vir_turned[...], coupling[v], preferred_element_type=F32)
        sigma_own[...] = total
        sigma_send[v] = total.astype(BF16)
        for way, peer in enumerate(others):
            remote(
                sigma_send.at[v, pl.ds(pl.multiple_of(peer * columns, 16), columns)],
                sigma_recv.at[v, way],
                sigma_sem.at[vectors],
                sigma_sem.at[v],
                (me, peer),
            ).start()
        out[v] = gaps[...] * trial[v] + sigma_own[pl.ds(pl.multiple_of(band * columns, 16), columns)]

    take_halves(0)
    drain(occ_tile.at[pl.ds(0, groups), pl.ds(0, width - piece)], occ_pass_sem.at[1])
    make_pairs(0, 0, width - piece)
    for step in range(groups - 2):
        take_corner(step)
        if step == groups - 3:
            for position in range(groups - 2, groups):
                take_corner(position)
        screen_far(0, step, early)
    drain(occ_tile.at[pl.ds(0, groups), pl.ds(0, piece)], occ_pass_sem.at[2])
    make_pairs(0, width - piece, piece)
    for step in range(groups - 2):
        screen_far(0, step, late, True)
        send_far(0, step)

    def both_far(v, step):
        screen_far(v, step, whole)
        send_far(v, step)

    sum_density()
    for v in range(1, vectors):
        take_halves(v)
        make_pairs(v, 0, width)
        for step in range(groups - 2):
            both_far(v, step)
    for step in range(groups - 2):
        gather_far(0, step)
    both_far(0, groups - 2)
    gather_far(0, groups - 2)
    for v in range(1, vectors):
        both_far(v, groups - 2)
        for step in range(groups - 2):
            gather_far(v, step)
    for v in range(vectors):
        send_own(v)
        if v == 0:
            for later in range(1, vectors):
                gather_far(later, groups - 2)
            make_potential()
        make_sigma(v)
    for v in range(vectors):
        drain(sigma_recv.at[v], sigma_sem.at[v])
        result = out[v]
        for way in range(bands - 1):
            result += sigma_recv[v, way].astype(F32)
        out[v] = result

    drain(sigma_recv, trial_sem.at[vectors])
    drain(sigma_recv, sigma_sem.at[vectors])
    drain(
        exch_tile.at[pl.ds(0, groups - 1), pl.ds(0, occupied // bands)], point_sem.at[groups]
    )
    drain(occ_tile.at[pl.ds(0, groups), pl.ds(0, width - piece)], occ_send_sem.at[0])
    drain(occ_tile.at[pl.ds(0, groups)], occ_pass_sem.at[0])
    drain(half_all.at[pl.ds(0, groups + 1)], half_send_sem.at[0])
    drain(dens_all.at[pl.ds(0, kpoints - 1)], dens_sem.at[0])
    drain(dens_band.at[pl.ds(0, bands - 1)], dens_band_sem.at[0])
    for v in range(vectors):
        drain(sums_slot.at[v, pl.ds(0, 2 * groups - 1)], sums_send_sem.at[v])
        for far in range(groups - 2):
            for owner_core in range(2):
                pl.when(passing(v, far_groups[far]))(half_pass(v, far, owner_core).wait_send)
    for copy, direct in direct_copies():
        pl.when(direct)(copy.wait_send)


def coupled_part(
    kpoints, bands, occ, vir, trial, occ_energy, vir_energy, coulomb, exch, table
):
    rows, occupied = occ.shape
    vectors, columns = trial.shape[:2]
    groups = kpoints // 2
    count = groups // 2
    block = rows // groups
    width = bands * rows // 2
    vmem = pl.BlockSpec(memory_space=pltpu.VMEM)
    hbm = pl.BlockSpec(memory_space=pltpu.HBM)
    dma = pltpu.SemaphoreType.DMA
    return pl.pallas_call(
        functools.partial(kernel, kpoints, bands, vectors),
        out_shape=pltpu.VMEM(trial.shape, F32),
        in_specs=[hbm] * 8,
        out_specs=vmem,
        scratch_shapes=[
            pltpu.VMEM(occ.shape, BF16),
            pltpu.VMEM(vir.shape, BF16),
            pltpu.VMEM(trial.shape, F32),
            pltpu.VMEM(occ_energy.shape, F32),
            pltpu.VMEM(vir_energy.shape, F32),
            pltpu.SMEM(table.shape, jnp.int32),
            pltpu.VMEM((columns, occupied), F32),
            pltpu.VMEM((kpoints, block, width), F32),
            pltpu.VMEM((vectors, bands * columns, occupied), BF16),
            pltpu.VMEM((bands * columns, rows), BF16),
            pltpu.VMEM((vectors, rows, occupied), BF16),
            pltpu.VMEM((kpoints, vectors * block, occupied), BF16),
            pltpu.VMEM((kpoints, width, occupied), BF16),
            pltpu.VMEM((kpoints, vectors, rows), F32),
            pltpu.VMEM((bands, vectors, rows), F32),
            pltpu.VMEM((rows, 128), F32),
            pltpu.VMEM(coulomb.shape, BF16),
            pltpu.VMEM((kpoints, block, width), BF16),
            pltpu.VMEM((kpoints, vectors * block, width), F32),
            pltpu.VMEM((vectors, groups - 1, 2, block, occupied), F32),
            pltpu.VMEM((vectors, groups, 2, block, occupied), BF16),
            pltpu.VMEM((vectors, 2 * groups + kpoints, block, occupied), BF16),
            pltpu.VMEM((vectors, rows, occupied), BF16),
            pltpu.VMEM((bands * columns, occupied), F32),
            pltpu.VMEM((vectors, bands * columns, occupied), BF16),
            pltpu.VMEM((vectors, bands - 1, columns, occupied), BF16),
            dma((8,)),
            dma((vectors + 1,)),
            dma((groups + 1,)),
            dma((1,)),
            dma((groups, 2)),
            dma((3,)),
            dma((1,)),
            dma((vectors, kpoints - 3)),
            dma((vectors, groups - 2, 2)),
            dma((count - 1, 2)),
            dma((2,)),
            dma((2,)),
            dma((vectors,)),
            dma((vectors, kpoints - 3)),
            dma((vectors + 1,)),
        ],
        compiler_params=pltpu.CompilerParams(
            collective_id=0, has_side_effects=True, vmem_limit_bytes=40 * 2**20
        ),
        name="coupled",
    )(
        *(
            pltpu.with_memory_space_constraint(given, pltpu.HBM)
            for given in (occ, vir, trial, occ_energy, vir_energy, coulomb, exch, table)
        )
    )


def per_device(
    occ_rows, vir_rows, trial_vectors, occ_energy, vir_energy, coulomb, exch_kernel, minus_table
):
    kpoints = lax.axis_size("ka")
    bands = lax.axis_size("band")
    trial_turned = jnp.swapaxes(trial_vectors[0], 1, 2)
    coupled = coupled_part(
        kpoints,
        bands,
        occ_rows[0],
        vir_rows[0],
        trial_turned,
        occ_energy,
        vir_energy,
        coulomb,
        exch_kernel,
        minus_table,
    )
    return jnp.swapaxes(coupled, 1, 2)[None]


def solution(mesh):
    in_specs = (
        P("ka", "band", None),
        P("ka", "band", None),
        P("ka", None, None, "band"),
        P("ka", None),
        P("ka", "band"),
        P("band", None),
        P(None, "band", None),
        P(),
    )
    out_specs = P("ka", None, None, "band")
    return jax.shard_map(
        per_device, mesh=mesh, in_specs=in_specs, out_specs=out_specs, check_vma=False
    )
```
